256 devices in a mesh: slab: 32 (over x, y, core), probe: 8 (over z).
Axes of the slice: x: 4, y: 4, z: 8, core: 2. Of those that a mesh axis runs over, the one named last changes fastest.
Arguments:
- probes: float32 [16, 3, 64, 128, 128], P('probe', None, 'slab'), may hold values from -50 to 50
- earlier: float32 [16, 3, 64, 128, 128], P(None, None, 'slab', 'probe'), may hold values from -16 to 16
- modulus: float32 [64, 128, 128], P('slab'), may hold values from 0.5 to 2
- tangent: float32 [6, 64, 128, 128], P(None, 'slab'), may hold values from -0.3 to 2, as said below
Outputs:
- basis: float32 [16, 3, 64, 128, 128], P('probe', None, 'slab')
- correlation: float32 [16, 16], replicated
The draws below stay inside these ranges and needn't reach their ends.
Inputs may be any that keep to these rules, and one draw needn't show every extreme that they name: `tangent`: entries 0 to 2 lie in 1 to 2, entries 3 to 5 in -0.3 to 0.3.
All inputs are finite; a program needn't handle non-finite values.
Results may differ from the reference program's by a relative error of at most 0.00014.
Values sent between devices are 32-bit elements; how exact they have to be, the bound alone decides.
No kernel may reach another device: no remote copies, remote signals or barrier semaphores. Data moves between devices by JAX's collectives and lax.ppermute only.
A program may use at most 64 MiB of HBM per device.

```python
import math
import jax
import jax.numpy as jnp
from jax import lax

NY = 128
NX = 128
EARLIER = 16
NZ = 64
PROBES = 16


def draw_probes(key, part):
    subkeys = jax.random.split(key, 3)
    extent = (PROBES, 3, NZ, NY, NX)
    column_scale = 10.0 ** jax.random.uniform(subkeys[1], (PROBES, 1, 1, 1, 1), jnp.float32, -0.5, 0.5)
    row_scale = 10.0 ** jax.random.uniform(subkeys[2], (1, 1, NZ, NY, 1), jnp.float32, -0.5, 0.5)
    values = jnp.clip(jax.random.normal(subkeys[0], extent, jnp.float32), -5.0, 5.0)
    return values * column_scale * row_scale


def draw_earlier(key, part):
    subkeys = jax.random.split(key, 2)
    extent = (EARLIER, 3, NZ, NY, NX)
    column_scale = 10.0 ** jax.random.uniform(subkeys[1], (EARLIER, 1, 1, 1, 1), jnp.float32, -0.5, 0.5)
    values = jnp.clip(jax.random.normal(subkeys[0], extent, jnp.float32), -5.0, 5.0)
    return values * column_scale


def draw_tangent(key, part):
    uniform_part = jax.random.uniform(key, (6, NZ, NY, NX), jnp.float32, 0.0, 1.0)
    diagonal_part = 1.0 + uniform_part[0:3]
    coupling = 0.6 * uniform_part[3:6] - 0.3
    return jnp.concatenate([diagonal_part, coupling], axis=0)


def levels(rng, shape, shards, least, largest):
    def one(dim, parts):
        draws = jax.random.uniform(jax.random.fold_in(jax.random.fold_in(rng, 6), dim), (parts,), jnp.float32, least / len(shards), largest / len(shards))
        return jnp.repeat(jnp.exp(draws), shape[dim] // parts).reshape((-1,) + (1,) * (len(shape) - dim - 1))

    gain = one(*shards[0])
    for cut in shards[1:]:
        gain = gain * one(*cut)
    return gain


def setup_inputs(seed: int = 0) -> dict:
    arg_keys = jax.random.split(jax.random.key(seed), 5)
    return {
        "probes": draw_probes(jax.random.fold_in(arg_keys[4], 71), 0),
        "earlier": draw_earlier(jax.random.fold_in(arg_keys[4], 71), 0),
        "modulus": jnp.clip(jnp.exp(math.log(2.0) - 1.3862944 * jax.random.uniform(arg_keys[2], (NZ, NY, NX), jnp.float32) ** levels(arg_keys[2], (NZ, NY, NX), ((0, 32),), -0.2, 0.2)), 0.5, 2.0),
        "tangent": draw_tangent(jax.random.fold_in(arg_keys[4], 71), 0),
    }


def scaled_tangent(vectors, modulus, tensor):
    planes = vectors.shape[2] - 2
    height = vectors.shape[3]
    breadth = vectors.shape[4]
    padded = jnp.pad(vectors, ((0, 0), (0, 0), (0, 0), (1, 1), (1, 1)))
    mod_pad = jnp.pad(modulus, ((0, 0), (1, 1), (1, 1)))
    centre = padded[:, :, 1:planes + 1, 1:height + 1, 1:breadth + 1]
    mod_centre = mod_pad[1:planes + 1, 1:height + 1, 1:breadth + 1]
    summed = jnp.zeros_like(centre)
    for step_z in (-1, 0, 1):
        for step_y in (-1, 0, 1):
            for step_x in (-1, 0, 1):
                reach = abs(step_z) + abs(step_y) + abs(step_x)
                if reach == 0:
                    continue
                weight = (0.3, 0.1, 0.05)[reach - 1]
                nearby = padded[:, :, 1 + step_z:planes + 1 + step_z, 1 + step_y:height + 1 + step_y, 1 + step_x:breadth + 1 + step_x]
                mod_near = mod_pad[1 + step_z:planes + 1 + step_z, 1 + step_y:height + 1 + step_y, 1 + step_x:breadth + 1 + step_x]
                edge_coef = 0.5 * weight * (mod_centre + mod_near)
                summed = summed + edge_coef * (centre - nearby)
    first_c = centre[:, 0]
    second_c = centre[:, 1]
    third_c = centre[:, 2]
    local_part = jnp.stack([tensor[0] * first_c + tensor[3] * second_c + tensor[4] * third_c, tensor[3] * first_c + tensor[1] * second_c + tensor[5] * third_c, tensor[4] * first_c + tensor[5] * second_c + tensor[2] * third_c], axis=1)
    return (summed + local_part - 8.0 * centre) / 8.0

def pad_planes(values):
    return jnp.pad(values, ((0, 0), (0, 0), (1, 1), (0, 0), (0, 0)))

def reference(probes, earlier, modulus, tangent):
    mod_padded = jnp.pad(modulus, ((1, 1), (0, 0), (0, 0)))

    def filter_one(single):
        single = single[None]
        first = scaled_tangent(pad_planes(single), mod_padded, tangent)
        second = scaled_tangent(pad_planes(first), mod_padded, tangent)
        return (2.0 * second - single)[0]
    filtered = lax.map(filter_one, probes)
    highest = lax.Precision.HIGHEST
    flat_y = filtered.reshape(filtered.shape[0], -1)
    flat_q = earlier.reshape(earlier.shape[0], -1)
    gram_earlier = jnp.dot(flat_q, flat_q.T, precision=highest)
    cross = jnp.dot(flat_q, flat_y.T, precision=highest)
    factor = jnp.linalg.cholesky(gram_earlier)
    coeff = jax.scipy.linalg.cho_solve((factor, True), cross)
    residue = flat_y - jnp.dot(coeff.T, flat_q, precision=highest)
    gram = jnp.dot(residue, residue.T, precision=highest)
    lower = jnp.linalg.cholesky(gram)
    scale = jnp.sqrt(jnp.float32(3 * NZ * NY * NX))
    basis = jax.scipy.linalg.solve_triangular(lower, residue, lower=True) * scale
    return (basis.reshape(filtered.shape), coeff * scale)
```

```python
import jax
import jax.numpy as jnp
from jax import lax
from jax.sharding import PartitionSpec as P


def padded_2(cells, sides, width):
    for axis, dim in sides:
        count = lax.axis_size(axis)
        ends = count - 1
        head = lax.slice_in_dim(cells, 0, width, axis=dim)
        tail = lax.slice_in_dim(cells, cells.shape[dim] - width, cells.shape[dim], axis=dim)
        cells = jnp.concatenate(
            [
                lax.ppermute(tail, axis, [(i, (i + 1) % count) for i in range(ends)]),
                cells,
                lax.ppermute(head, axis, [((i + 1) % count, i) for i in range(ends)]),
            ],
            axis=dim,
        )
    return cells


def scaled_tangent(vectors, modulus, tensor):
    planes = vectors.shape[2] - 2
    height = vectors.shape[3]
    breadth = vectors.shape[4]
    padded = jnp.pad(vectors, ((0, 0), (0, 0), (0, 0), (1, 1), (1, 1)))
    mod_pad = jnp.pad(modulus, ((0, 0), (1, 1), (1, 1)))
    centre = padded[:, :, 1 : planes + 1, 1 : height + 1, 1 : breadth + 1]
    mod_centre = mod_pad[1 : planes + 1, 1 : height + 1, 1 : breadth + 1]
    summed = jnp.zeros_like(centre)
    for step_z in (-1, 0, 1):
        for step_y in (-1, 0, 1):
            for step_x in (-1, 0, 1):
                reach = abs(step_z) + abs(step_y) + abs(step_x)
                if reach == 0:
                    continue
                weight = (0.3, 0.1, 0.05)[reach - 1]
                nearby = padded[
                    :,
                    :,
                    1 + step_z : planes + 1 + step_z,
                    1 + step_y : height + 1 + step_y,
                    1 + step_x : breadth + 1 + step_x,
                ]
                mod_near = mod_pad[
                    1 + step_z : planes + 1 + step_z,
                    1 + step_y : height + 1 + step_y,
                    1 + step_x : breadth + 1 + step_x,
                ]
                edge_coef = 0.5 * weight * (mod_centre + mod_near)
                summed = summed + edge_coef * (centre - nearby)
    first_c = centre[:, 0]
    second_c = centre[:, 1]
    third_c = centre[:, 2]
    local_part = jnp.stack(
        [
            tensor[0] * first_c + tensor[3] * second_c + tensor[4] * third_c,
            tensor[3] * first_c + tensor[1] * second_c + tensor[5] * third_c,
            tensor[4] * first_c + tensor[5] * second_c + tensor[2] * third_c,
        ],
        axis=1,
    )
    return (summed + local_part - 8.0 * centre) / 8.0


def sum_over(block, axis):
    count = lax.axis_size(axis)
    copies = jnp.broadcast_to(block[None], (count,) + block.shape)
    return jnp.sum(lax.all_to_all(copies, axis, 0, 0, tiled=True), axis=0)


def body(probes, earlier, modulus, tangent):
    depth = probes.shape[2]
    slabs = lax.axis_size("slab")
    highest = lax.Precision.HIGHEST
    ext_probe, ext_mod = (
        padded_2(probes, (("slab", 2),), 1),
        padded_2(modulus[None, None], (("slab", 2),), 1),
    )
    mod_wide = ext_mod[0, 0]
    first = scaled_tangent(ext_probe, mod_wide, tangent)
    ext_first = padded_2(first, (("slab", 2),), 1)
    second = scaled_tangent(ext_first, mod_wide, tangent)
    filtered = 2.0 * second - probes
    rows_y = lax.all_to_all(filtered, "probe", split_axis=3, concat_axis=0, tiled=True)
    kept = earlier.shape[0]
    both = jnp.concatenate([earlier, rows_y], axis=0)
    scale = jnp.sqrt(jnp.float32(3 * depth * slabs * probes.shape[3] * probes.shape[4]))
    dims = (1, 2, 3, 4)
    gram = lax.dot_general(both, both, ((dims, dims), ((), ())), precision=highest)
    total = gram.shape[0]
    gram = gram.reshape(8, total * total // 8)
    gram = sum_over(sum_over(gram, "slab"), "probe").reshape(total, total)
    factor = jnp.linalg.cholesky(gram)
    inverse = jax.scipy.linalg.solve_triangular(factor, jnp.eye(total, dtype=jnp.float32), lower=True)
    coeff = jnp.dot(inverse[:kept, :kept].T, factor[kept:, :kept].T, precision=highest)
    basis_rows = lax.dot_general(
        inverse[kept:] * scale, both, (((1,), (0,)), ((), ())), precision=highest
    )
    basis = lax.all_to_all(basis_rows, "probe", split_axis=0, concat_axis=3, tiled=True)
    return (basis, coeff * scale)


def solution(mesh):
    in_specs = (
        P("probe", None, "slab", None, None),
        P(None, None, "slab", "probe", None),
        P("slab", None, None),
        P(None, "slab", None, None),
    )
    out_specs = (P("probe", None, "slab", None, None), P())
    return jax.shard_map(body, mesh=mesh, in_specs=in_specs, out_specs=out_specs, check_vma=False)
```

```python
import math

import jax
import jax.numpy as jnp
from jax import lax
from jax.experimental import pallas as pl
from jax.experimental.pallas import tpu as pltpu
from jax.sharding import Mesh
from jax.sharding import PartitionSpec as P

STRIP = 16
PART = 0.05 / 16.0


def rows_at(ref, lead, start, shift, height):
    first = start + shift
    if first < 0:
        block = pltpu.roll(ref[lead + (pl.ds(0, STRIP), slice(None))], 1, 0)
        row = lax.broadcasted_iota(jnp.int32, block.shape, 0)
        return jnp.where(row == 0, 0.0, block)
    if first + STRIP > height:
        block = pltpu.roll(ref[lead + (pl.ds(height - STRIP, STRIP), slice(None))], STRIP - 1, 0)
        row = lax.broadcasted_iota(jnp.int32, block.shape, 0)
        return jnp.where(row == STRIP - 1, 0.0, block)
    return ref[lead + (pl.ds(first, STRIP), slice(None))]


def across(block):
    breadth = block.shape[1]
    lane = lax.broadcasted_iota(jnp.int32, block.shape, 1)
    left = jnp.where(lane == 0, 0.0, pltpu.roll(block, 1, 1))
    right = jnp.where(lane == breadth - 1, 0.0, pltpu.roll(block, breadth - 1, 1))
    return left + right


def outer_sum(mid, above, below):
    tall = (mid + mid) + (above + below)
    both = tall + mid
    return across(tall) + (both + both)


def full_sum(mid, pair_y, side, side_y):
    near = pair_y + side
    six = 6.0 * mid
    inner = (near + near) + (six + side_y)
    rest = inner + (near - six)
    return across(inner) + (rest + rest)


def combine(diag, off, fields):
    a, b, c = fields
    return (
        diag[0] * a + off[0] * b + off[1] * c,
        off[0] * a + diag[1] * b + off[2] * c,
        off[1] * a + off[2] * b + diag[2] * c,
    )


def partial_kernel(probes_far, modulus_far, tangent_far, down, up, probes, modulus, tangent, prod, sems):
    count = probes.shape[0]
    height = probes.shape[3]
    pairs = ((modulus_far, modulus), (probes_far, probes), (tangent_far, tangent))
    copies = [pltpu.make_async_copy(src, dst, sems.at[n]) for n, (src, dst) in enumerate(pairs)]
    for copy in copies:
        copy.start()
    copies[0].wait()
    copies[1].wait()
    for z in range(2):
        for k in range(count):
            for i in range(3):
                prod[z * 3 * count + 3 * k + i] = probes[k, i, z] * modulus[z]
    copies[2].wait()
    for z, out in ((0, down), (1, up)):
        other = 1 - z
        for s in range(0, height, STRIP):
            here = pl.ds(s, STRIP)

            def mod(plane, shift):
                return rows_at(modulus, (plane,), s, shift, height)

            m = mod(z, 0)
            side = mod(other, 0)
            neighbours = full_sum(m, mod(z, -1) + mod(z, 1), side, mod(other, -1) + mod(other, 1))
            common = (3.4 / 16.0) * m + PART * neighbours - 1.0
            diag = [common + 0.125 * tangent[i, z, here, :] for i in range(3)]
            off = [0.125 * tangent[3 + i, z, here, :] for i in range(3)]
            scaled = PART * m
            out[6 * count, here, :] = m
            for k in range(count):
                values = [probes[k, i, z, here, :] for i in range(3)]
                mixed = combine(diag, off, values)
                for i in range(3):
                    def val(plane, shift):
                        return rows_at(probes, (k, i, plane), s, shift, height)

                    def pro(plane, shift):
                        return rows_at(prod, (plane * 3 * count + 3 * k + i,), s, shift, height)

                    first = full_sum(values[i], val(z, -1) + val(z, 1), val(other, 0), val(other, -1) + val(other, 1))
                    second = full_sum(pro(z, 0), pro(z, -1) + pro(z, 1), pro(other, 0), pro(other, -1) + pro(other, 1))
                    out[3 * k + i, here, :] = values[i]
                    out[3 * count + 3 * k + i, here, :] = mixed[i] - scaled * first - PART * second


def filter_kernel(lo, down, up, hi, tangent, out, once, prod, sums, products, prior):
    planes = (lo, down, up, hi)
    total = (lo.shape[0] - 1) // 2
    count = total // 3
    height = lo.shape[1]
    for z in range(4):
        for n in range(total):
            prior[z * total + n] = planes[z][n] * planes[z][2 * total]
    for source, target in ((0, 1), (1, 0), (2, 3), (3, 2)):
        src = planes[source]
        dst = planes[target]
        for s in range(0, height, STRIP):
            here = pl.ds(s, STRIP)

            def at(ref, n, shift):
                return rows_at(ref, (n,), s, shift, height)

            m = dst[2 * total, here, :]
            weight = PART * outer_sum(at(src, 2 * total, 0), at(src, 2 * total, -1), at(src, 2 * total, 1))
            scaled = PART * m
            for n in range(total):
                first = outer_sum(at(src, n, 0), at(src, n, -1), at(src, n, 1))
                j = source * total + n
                second = outer_sum(at(prior, j, 0), at(prior, j, -1), at(prior, j, 1))
                value = dst[total + n, here, :] + weight * dst[n, here, :] - scaled * first - PART * second
                if target in (0, 3):
                    value = jnp.where(m > 0.0, value, 0.0)
                once[target * total + n, here, :] = value
                prod[target * total + n, here, :] = value * m
    for z in (1, 2):
        for n in range(total):
            sums[(z - 1) * total + n] = once[(z - 1) * total + n] + once[(z + 1) * total + n]
            products[(z - 1) * total + n] = prod[(z - 1) * total + n] + prod[(z + 1) * total + n]
    for z in (1, 2):
        plane = planes[z]
        for s in range(0, height, STRIP):
            here = pl.ds(s, STRIP)

            def at(ref, n, shift):
                return rows_at(ref, (n,), s, shift, height)

            def mod(p, shift):
                return rows_at(planes[p], (2 * total,), s, shift, height)

            m = mod(z, 0)
            side = [mod(z - 1, d) + mod(z + 1, d) for d in (-1, 0, 1)]
            neighbours = full_sum(m, mod(z, -1) + mod(z, 1), side[1], side[0] + side[2])
            common = (6.8 / 16.0) * m + (2.0 * PART) * neighbours - 2.0
            diag = [common + 0.25 * tangent[i, z - 1, here, :] for i in range(3)]
            off = [0.25 * tangent[3 + i, z - 1, here, :] for i in range(3)]
            scaled = (2.0 * PART) * m
            for k in range(count):
                base = z * total + 3 * k
                mixed = combine(diag, off, [once[base + i, here, :] for i in range(3)])
                for i in range(3):
                    n = base + i
                    j = n - total
                    first = full_sum(at(once, n, 0), at(once, n, -1) + at(once, n, 1), at(sums, j, 0), at(sums, j, -1) + at(sums, j, 1))
                    second = full_sum(at(prod, n, 0), at(prod, n, -1) + at(prod, n, 1), at(products, j, 0), at(products, j, -1) + at(products, j, 1))
                    value = mixed[i] - scaled * first - (2.0 * PART) * second - plane[3 * k + i, here, :]
                    out[s // STRIP, k, i, z - 1] = value


VM = pl.BlockSpec(memory_space=pltpu.VMEM)


def partial_call(probes, modulus, tangent, **kw):
    count, _, _, height, breadth = probes.shape
    pack = pltpu.VMEM((6 * count + 1, height, breadth), jnp.float32)
    return pl.pallas_call(
        partial_kernel,
        out_shape=(pack, pack),
        in_specs=[pl.BlockSpec(memory_space=pl.ANY)] * 3,
        out_specs=(VM, VM),
        scratch_shapes=[pltpu.VMEM(a.shape, jnp.float32) for a in (probes, modulus, tangent)]
        + [pltpu.VMEM((6 * count, height, breadth), jnp.float32), pltpu.SemaphoreType.DMA((3,))],
        compiler_params=pltpu.CompilerParams(vmem_limit_bytes=20 << 20),
        name="partial",
        **kw,
    )(probes, modulus, tangent)


def filter_call(lo, down, up, hi, tangent, **kw):
    packed, height, breadth = lo.shape
    total = (packed - 1) // 2
    count = total // 3
    plane = lambda n: pltpu.VMEM((n, height, breadth), jnp.float32)
    return pl.pallas_call(
        filter_kernel,
        out_shape=pltpu.VMEM((height // STRIP, count, 3, 2, STRIP, breadth), jnp.float32),
        in_specs=[VM] * 5,
        out_specs=VM,
        scratch_shapes=[plane(4 * total), plane(4 * total), plane(2 * total), plane(2 * total), plane(4 * total)],
        compiler_params=pltpu.CompilerParams(vmem_limit_bytes=24 << 20),
        name="filter",
        **kw,
    )(*(pltpu.with_memory_space_constraint(a, pltpu.VMEM) for a in (lo, down, up, hi, tangent)))


def sum_over(block, axes, count):
    copies = jnp.broadcast_to(block[None], (count,) + block.shape)
    return jnp.sum(lax.all_to_all(copies, axes, 0, 0, tiled=True), axis=0)


def body(probes, earlier, modulus, tangent, slabs, columns, scale):
    highest = lax.Precision.HIGHEST
    down, up = partial_call(probes, modulus, tangent)
    places = ("x", "y", "core")
    ends = slabs - 1
    lo = lax.ppermute(up, places, [(i, i + 1) for i in range(ends)])
    hi = lax.ppermute(down, places, [(i + 1, i) for i in range(ends)])
    filtered = filter_call(lo, down, up, hi, tangent)
    filtered, earlier = lax.optimization_barrier((filtered, earlier))
    rows_y = lax.all_to_all(filtered, "probe", 0, 0, tiled=True)
    rows_y, earlier = lax.optimization_barrier((rows_y, earlier))
    kept = earlier.shape[0]
    both = jnp.concatenate([earlier, rows_y.reshape(earlier.shape)], axis=0)
    dims = (1, 2, 3, 4)
    gram = lax.dot_general(both, both, ((dims, dims), ((), ())), precision=highest)
    total = gram.shape[0]
    gram = gram.reshape(8, total * total // 8)
    gram = sum_over(gram, ("probe", "core"), 2 * columns)
    gram = sum_over(gram, ("x", "y"), slabs // 2).reshape(total, total)
    factor = jnp.linalg.cholesky(gram)
    inverse = jax.scipy.linalg.solve_triangular(factor, jnp.eye(total, dtype=jnp.float32), lower=True)
    coeff = jnp.dot(inverse[:kept, :kept].T, factor[kept:, :kept].T, precision=highest)
    basis_rows = lax.dot_general(
        inverse[kept:] * scale, both, (((1,), (0,)), ((), ())), precision=highest
    ).reshape(filtered.shape)
    correlation = coeff * scale
    basis_rows, correlation = lax.optimization_barrier((basis_rows, correlation))
    blocks = lax.all_to_all(basis_rows, "probe", 0, 0, tiled=True)
    basis = jnp.transpose(blocks, (1, 2, 3, 0, 4, 5)).reshape(probes.shape)
    return (basis, correlation)


def solution(mesh):
    slabs = mesh.shape["slab"]
    columns = mesh.shape["probe"]
    side = math.isqrt(slabs // 2)
    wide = Mesh(mesh.devices.reshape(side, side, 2, columns), ("x", "y", "core", "probe"))
    slab = ("x", "y", "core")
    in_specs = (
        P("probe", None, slab, None, None),
        P(None, None, slab, "probe", None),
        P(slab, None, None),
        P(None, slab, None, None),
    )
    out_specs = (P("probe", None, slab, None, None), P())

    def step(probes, earlier, modulus, tangent):
        length = math.prod(probes.shape[1:])
        scale = jnp.sqrt(jnp.float32(length))
        inner = lambda *parts: body(*parts, slabs, columns, scale)
        return jax.shard_map(inner, mesh=wide, in_specs=in_specs, out_specs=out_specs, check_vma=False)(
            probes, earlier, modulus, tangent
        )

    return step
```

```python
import math

import jax
import jax.numpy as jnp
from jax import lax
from jax.experimental import pallas as pl
from jax.experimental.pallas import tpu as pltpu
from jax.sharding import Mesh
from jax.sharding import PartitionSpec as P

STRIP = 16
PART = 0.05 / 16.0


def rows_at(ref, lead, start, shift, height):
    first = start + shift
    if first < 0:
        block = pltpu.roll(ref[lead + (pl.ds(0, STRIP), slice(None))], 1, 0)
        row = lax.broadcasted_iota(jnp.int32, block.shape, 0)
        return jnp.where(row == 0, 0.0, block)
    if first + STRIP > height:
        block = pltpu.roll(ref[lead + (pl.ds(height - STRIP, STRIP), slice(None))], STRIP - 1, 0)
        row = lax.broadcasted_iota(jnp.int32, block.shape, 0)
        return jnp.where(row == STRIP - 1, 0.0, block)
    return ref[lead + (pl.ds(first, STRIP), slice(None))]


def across(block):
    breadth = block.shape[1]
    lane = lax.broadcasted_iota(jnp.int32, block.shape, 1)
    left = jnp.where(lane == 0, 0.0, pltpu.roll(block, 1, 1))
    right = jnp.where(lane == breadth - 1, 0.0, pltpu.roll(block, breadth - 1, 1))
    return left + right


def outer_sum(mid, above, below):
    tall = (mid + mid) + (above + below)
    both = tall + mid
    return across(tall) + (both + both)


def full_sum(mid, pair_y, side, side_y):
    near = pair_y + side
    six = 6.0 * mid
    inner = (near + near) + (six + side_y)
    rest = inner + (near - six)
    return across(inner) + (rest + rest)


def combine(diag, off, fields):
    a, b, c = fields
    return (
        diag[0] * a + off[0] * b + off[1] * c,
        off[0] * a + diag[1] * b + off[2] * c,
        off[1] * a + off[2] * b + diag[2] * c,
    )


def partial_kernel(place, probes_far, modulus_far, tangent_far, far, near, probes, modulus, tangent, prod, sems):
    count = probes.shape[0]
    height = probes.shape[3]
    core = place[0]
    copies = []
    for z, plane in ((0, core), (1, 1 - core)):
        triples = (
            (modulus_far.at[pl.ds(plane, 1)], modulus.at[pl.ds(z, 1)]),
            (probes_far.at[:, :, pl.ds(plane, 1)], probes.at[:, :, pl.ds(z, 1)]),
            (tangent_far.at[:, pl.ds(plane, 1)], tangent.at[:, pl.ds(z, 1)]),
        )
        copies.append([pltpu.make_async_copy(src, dst, sems.at[z, n]) for n, (src, dst) in enumerate(triples)])
    for n in range(3):
        copies[0][n].start()
        copies[1][n].start()
    for n in range(2):
        copies[0][n].wait()
        copies[1][n].wait()
    for z in range(2):
        for k in range(count):
            for i in range(3):
                prod[z * 3 * count + 3 * k + i] = probes[k, i, z] * modulus[z]
    copies[0][2].wait()
    copies[1][2].wait()
    for z, out in ((0, far), (1, near)):
        other = 1 - z
        for s in range(0, height, STRIP):
            here = pl.ds(s, STRIP)

            def mod(plane, shift):
                return rows_at(modulus, (plane,), s, shift, height)

            m = mod(z, 0)
            side = mod(other, 0)
            neighbours = full_sum(m, mod(z, -1) + mod(z, 1), side, mod(other, -1) + mod(other, 1))
            common = (3.4 / 16.0) * m + PART * neighbours - 1.0
            diag = [common + 0.125 * tangent[i, z, here, :] for i in range(3)]
            off = [0.125 * tangent[3 + i, z, here, :] for i in range(3)]
            scaled = PART * m
            out[6 * count, here, :] = m
            for k in range(count):
                values = [probes[k, i, z, here, :] for i in range(3)]
                mixed = combine(diag, off, values)
                for i in range(3):
                    def val(plane, shift):
                        return rows_at(probes, (k, i, plane), s, shift, height)

                    def pro(plane, shift):
                        return rows_at(prod, (plane * 3 * count + 3 * k + i,), s, shift, height)

                    first = full_sum(values[i], val(z, -1) + val(z, 1), val(other, 0), val(other, -1) + val(other, 1))
                    second = full_sum(pro(z, 0), pro(z, -1) + pro(z, 1), pro(other, 0), pro(other, -1) + pro(other, 1))
                    out[3 * k + i, here, :] = values[i]
                    out[3 * count + 3 * k + i, here, :] = mixed[i] - scaled * first - PART * second


def filter_kernel(place, lo, down, up, hi, tangent_far, out, tangent, once, prod, sums, products, prior, sems):
    planes = (lo, down, up, hi)
    core = place[0]
    copies = [
        pltpu.make_async_copy(tangent_far.at[:, pl.ds(plane, 1)], tangent.at[:, pl.ds(z, 1)], sems.at[z])
        for z, plane in ((0, core), (1, 1 - core))
    ]
    for copy in copies:
        copy.start()
    total = (lo.shape[0] - 1) // 2
    count = total // 3
    height = lo.shape[1]
    blocks = height // STRIP
    for z in range(4):
        for n in range(total):
            prior[z * total + n] = planes[z][n] * planes[z][2 * total]
    for source, target in ((0, 1), (1, 0), (2, 3), (3, 2)):
        src = planes[source]
        dst = planes[target]
        for s in range(0, height, STRIP):
            here = pl.ds(s, STRIP)

            def at(ref, n, shift):
                return rows_at(ref, (n,), s, shift, height)

            m = dst[2 * total, here, :]
            weight = PART * outer_sum(at(src, 2 * total, 0), at(src, 2 * total, -1), at(src, 2 * total, 1))
            scaled = PART * m
            for n in range(total):
                first = outer_sum(at(src, n, 0), at(src, n, -1), at(src, n, 1))
                j = source * total + n
                second = outer_sum(at(prior, j, 0), at(prior, j, -1), at(prior, j, 1))
                value = dst[total + n, here, :] + weight * dst[n, here, :] - scaled * first - PART * second
                if target in (0, 3):
                    value = jnp.where(m > 0.0, value, 0.0)
                once[target * total + n, here, :] = value
                prod[target * total + n, here, :] = value * m
    for z in (1, 2):
        for n in range(total):
            sums[(z - 1) * total + n] = once[(z - 1) * total + n] + once[(z + 1) * total + n]
            products[(z - 1) * total + n] = prod[(z - 1) * total + n] + prod[(z + 1) * total + n]
    for copy in copies:
        copy.wait()
    for z, depth in ((1, core), (2, 1 - core)):
        plane = planes[z]
        for s in range(0, height, STRIP):
            here = pl.ds(s, STRIP)

            def at(ref, n, shift):
                return rows_at(ref, (n,), s, shift, height)

            def mod(p, shift):
                return rows_at(planes[p], (2 * total,), s, shift, height)

            m = mod(z, 0)
            side = [mod(z - 1, d) + mod(z + 1, d) for d in (-1, 0, 1)]
            neighbours = full_sum(m, mod(z, -1) + mod(z, 1), side[1], side[0] + side[2])
            common = (6.8 / 16.0) * m + (2.0 * PART) * neighbours - 2.0
            diag = [common + 0.25 * tangent[i, z - 1, here, :] for i in range(3)]
            off = [0.25 * tangent[3 + i, z - 1, here, :] for i in range(3)]
            scaled = (2.0 * PART) * m
            turn = lax.rem(s // STRIP + blocks - place[1], blocks)
            for k in range(count):
                base = z * total + 3 * k
                mixed = combine(diag, off, [once[base + i, here, :] for i in range(3)])
                for i in range(3):
                    n = base + i
                    j = n - total
                    first = full_sum(at(once, n, 0), at(once, n, -1) + at(once, n, 1), at(sums, j, 0), at(sums, j, -1) + at(sums, j, 1))
                    second = full_sum(at(prod, n, 0), at(prod, n, -1) + at(prod, n, 1), at(products, j, 0), at(products, j, -1) + at(products, j, 1))
                    value = mixed[i] - scaled * first - (2.0 * PART) * second - plane[3 * k + i, here, :]
                    out[turn, k, i, depth] = value


def split(block):
    high = block.astype(jnp.bfloat16)
    rest = block - high.astype(jnp.float32)
    middle = rest.astype(jnp.bfloat16)
    low = (rest - middle.astype(jnp.float32)).astype(jnp.bfloat16)
    return high, middle, low


def gram_kernel(place, earlier, *refs):
    chunks, out, stack, tall = refs[:-3], refs[-3], refs[-2], refs[-1]
    length, wide = stack.shape[0], stack.shape[1]
    total = wide // 3
    kept = earlier.shape[0] // length
    turns = out_turns(chunks)
    count = sum(c.shape[0] for c, _, _ in turns) * 1 // max(t[1] + 1 for t in turns)
    blocks = (total - kept) // count
    for j in range(kept):
        tall[pl.ds(j, length, stride=total), :] = earlier[j * length : (j + 1) * length, :]
    for chunk, turn, first in turns:
        source = lax.rem(place[1] + blocks - turn, blocks)
        for p in range(chunk.shape[0]):
            row = kept + count * source + first + p
            tall[pl.ds(row, length, stride=total), :] = chunk[p]

    def step(r, gram):
        halves = []
        for h in range(2):
            block = tall[pl.ds((2 * r + h) * total, total), :]
            parts = jnp.concatenate(split(block), axis=0)
            stack[2 * r + h] = parts
            halves.append(parts)
        both = jnp.concatenate(halves, axis=1)
        return gram + lax.dot_general(both, both, (((1,), (1,)), ((), ())), preferred_element_type=jnp.float32)

    gram = lax.fori_loop(0, length // 2, step, jnp.zeros((wide, wide), jnp.float32), unroll=4)
    rows = (gram[:total] + gram[total : 2 * total]) + gram[2 * total :]
    gram = (rows[:, :total] + rows[:, total : 2 * total]) + rows[:, 2 * total :]
    packed = jnp.concatenate([gram[8 * q : 8 * q + 8] for q in range(total // 8)], axis=1)
    for n in range(out.shape[0]):
        out[n] = packed


def out_turns(chunks):
    half = (len(chunks) - 1) // 2
    listed = []
    for n, chunk in enumerate(chunks):
        if n < half:
            listed.append((chunk, n, 0))
        elif n == half:
            listed.append((chunk, half, 0))
        elif n == half + 1:
            listed.append((chunk, half, chunks[half].shape[0]))
        else:
            listed.append((chunk, n - 1, 0))
    return listed


def finish_kernel(place, copies, stack, scale, out, correlation):
    length, wide = stack.shape[0], stack.shape[1]
    total = wide // 3
    kept = total // 2
    made = total - kept
    summed = copies[0]
    for n in range(1, copies.shape[0]):
        summed = summed + copies[n]
    gram = jnp.concatenate([summed[:, total * q : total * q + total] for q in range(total // 8)], axis=0)
    row = lax.broadcasted_iota(jnp.int32, (total, total), 0)
    column = lax.broadcasted_iota(jnp.int32, (total, total), 1)
    unit = jnp.where(row == column, 1.0, 0.0)
    work = jnp.concatenate([gram, unit, jnp.zeros((total, 128 - 2 * total), jnp.float32)], axis=1)
    below = lax.broadcasted_iota(jnp.int32, (total, 1), 0)
    pivots = jnp.zeros((total, 1), jnp.float32)
    factor = scale[0]
    for k in range(total):
        if k == kept:
            correlation[...] = -factor * work[kept:, total : total + kept]
        pivot = work[k : k + 1, k : k + 1]
        ratio = jnp.where(below > k, work[:, k : k + 1] / pivot, 0.0)
        pivots = jnp.where(below == k, pivot, pivots)
        work = work - ratio * work[k : k + 1, :]
    weights = factor * work[kept:, total : 2 * total] * lax.rsqrt(pivots[kept:])
    count = made // out_blocks(out, length, made)
    slot = lax.broadcasted_iota(jnp.int32, (made, made), 0)
    source = lax.broadcasted_iota(jnp.int32, (made, made), 1)
    moved = slot + count * place[1]
    moved = jnp.where(moved >= made, moved - made, moved)
    turn = jnp.where(moved == source, 1.0, 0.0)
    weights = jnp.dot(turn, weights, precision=lax.Precision.HIGHEST)
    high, middle, low = split(weights)
    left = jnp.concatenate([jnp.concatenate([part] * 3, axis=1) for part in (high, middle, low)], axis=0)
    for r in range(0, length, 2):
        both = jnp.concatenate([stack[r], stack[r + 1]], axis=1)
        wide_rows = lax.dot_general(left, both, (((1,), (0,)), ((), ())), preferred_element_type=jnp.float32)
        rows = (wide_rows[:made] + wide_rows[made : 2 * made]) + wide_rows[2 * made :]
        for h in range(2):
            out[pl.ds(r + h, made, stride=length), :] = rows[:, 128 * h : 128 * h + 128]


def out_blocks(out, length, made):
    return COLUMNS


COLUMNS = 8


def spread_kernel(place, *refs):
    blocks, out, sems = refs[:-2], refs[-2], refs[-1]
    turns = len(blocks) - 1
    copies = []
    for n, (block, k, first) in enumerate(out_turns(blocks)):
        source = lax.rem(place[1] + turns - k, turns)
        target = out.at[pl.ds(first, block.shape[0]), :, :, pl.ds(source * STRIP, STRIP), :]
        copies.append(pltpu.make_async_copy(block, target, sems.at[n]))
    for copy in copies:
        copy.start()
    for copy in copies:
        copy.wait()


VM = pl.BlockSpec(memory_space=pltpu.VMEM)
SM = pl.BlockSpec(memory_space=pltpu.SMEM)
FAR = pl.BlockSpec(memory_space=pltpu.HBM)


def near_chip(*arrays):
    return tuple(pltpu.with_memory_space_constraint(a, pltpu.VMEM) for a in arrays)


def in_far(*arrays):
    return tuple(pltpu.with_memory_space_constraint(a, pltpu.HBM) for a in arrays)


def partial_call(place, probes, modulus, tangent):
    count, _, _, height, breadth = probes.shape
    pack = pltpu.VMEM((6 * count + 1, height, breadth), jnp.float32)
    return pl.pallas_call(
        partial_kernel,
        out_shape=(pack, pack),
        in_specs=[SM] + [FAR] * 3,
        out_specs=(VM, VM),
        scratch_shapes=[pltpu.VMEM(a.shape, jnp.float32) for a in (probes, modulus, tangent)]
        + [pltpu.VMEM((6 * count, height, breadth), jnp.float32), pltpu.SemaphoreType.DMA((2, 3))],
        compiler_params=pltpu.CompilerParams(vmem_limit_bytes=20 << 20),
        name="partial",
    )(place, *in_far(probes, modulus, tangent))


def filter_call(place, lo, down, up, hi, tangent):
    packed, height, breadth = lo.shape
    total = (packed - 1) // 2
    count = total // 3
    plane = lambda n: pltpu.VMEM((n, height, breadth), jnp.float32)
    return pl.pallas_call(
        filter_kernel,
        out_shape=pltpu.VMEM((height // STRIP, count, 3, 2, STRIP, breadth), jnp.float32),
        in_specs=[SM] + [VM] * 4 + [FAR],
        out_specs=VM,
        scratch_shapes=[pltpu.VMEM(tangent.shape, jnp.float32), plane(4 * total), plane(4 * total), plane(2 * total), plane(2 * total), plane(4 * total)]
        + [pltpu.SemaphoreType.DMA((2,))],
        compiler_params=pltpu.CompilerParams(vmem_limit_bytes=24 << 20),
        name="filter",
    )(place, *near_chip(lo, down, up, hi), *in_far(tangent))


def gram_call(place, earlier, chunks, blocks, copies):
    kept = earlier.shape[0]
    breadth = earlier.shape[-1]
    length = math.prod(earlier.shape[1:-1])
    total = kept + chunks[0].shape[0] * blocks
    flat = [c.reshape(c.shape[0], length, breadth) for c in chunks]
    return pl.pallas_call(
        gram_kernel,
        out_shape=(
            pltpu.VMEM((copies, 8, total * total // 8), jnp.float32),
            pltpu.VMEM((length, 3 * total, breadth), jnp.bfloat16),
        ),
        in_specs=[SM] + [VM] * (1 + len(chunks)),
        out_specs=(VM, VM),
        scratch_shapes=[pltpu.VMEM((length * total, breadth), jnp.float32)],
        compiler_params=pltpu.CompilerParams(vmem_limit_bytes=16 << 20),
        name="gram",
    )(place, *near_chip(earlier.reshape(kept * length, breadth), *flat))


def finish_call(place, copies, stack, scale):
    length, wide, breadth = stack.shape
    half = wide // 6
    return pl.pallas_call(
        finish_kernel,
        out_shape=(
            pltpu.VMEM((half * length, breadth), jnp.float32),
            jax.ShapeDtypeStruct((half, half), jnp.float32),
        ),
        in_specs=[SM, VM, VM, SM],
        out_specs=(VM, VM),
        compiler_params=pltpu.CompilerParams(vmem_limit_bytes=16 << 20),
        name="finish",
    )(place, *near_chip(copies, stack), scale)


def spread_call(place, blocks):
    count, parts, depth, strip, breadth = blocks[0].shape
    return pl.pallas_call(
        spread_kernel,
        out_shape=jax.ShapeDtypeStruct((count, parts, depth, strip * (len(blocks) - 1), breadth), jnp.float32),
        in_specs=[SM] + [VM] * len(blocks),
        out_specs=FAR,
        scratch_shapes=[pltpu.SemaphoreType.DMA((len(blocks),))],
        compiler_params=pltpu.CompilerParams(vmem_limit_bytes=8 << 20),
        name="spread",
    )(place, *near_chip(*blocks))


def shift(block, by, columns):
    return lax.ppermute(block, "probe", [(j, (j + by) % columns) for j in range(columns)])


def exchange(parts, columns):
    half = columns // 2
    cut = parts[half].shape[0] // 2
    got = [parts[0]] + [None] * (columns - 1)
    back = shift(parts[half][cut:], -(half // 2), columns)
    ahead = shift(parts[half][:cut], half, columns)
    for k in range(half - 1, 0, -1):
        got[k] = shift(parts[k], k, columns)
        got[columns - k] = shift(parts[columns - k], columns - k, columns)
        if k == half - 1:
            back = shift(back, half // 2 - half, columns)
    return got[:half] + [ahead, back] + got[half + 1 :]


def body(probes, earlier, modulus, tangent, slabs, columns, scale):
    place = jnp.stack([lax.axis_index("core"), lax.axis_index("probe")]).astype(jnp.int32)
    far, near = partial_call(place, probes, modulus, tangent)
    places = ("x", "y", "core")
    outer = [(i, i + 1) for i in range(1, slabs - 1, 2)] + [(i, i - 1) for i in range(2, slabs, 2)]
    got_far = lax.ppermute(far, places, outer)
    got_near = lax.ppermute(near, "core", [(0, 1), (1, 0)])
    filtered = filter_call(place, got_far, far, near, got_near, tangent)
    got = exchange([filtered[k] for k in range(columns)], columns)
    copies, stack = gram_call(place, earlier, got, columns, 2 * columns)
    copies = lax.all_to_all(copies, ("probe", "core"), 0, 0, tiled=True)
    copies = jnp.broadcast_to(jnp.sum(copies, axis=0, keepdims=True), (slabs // 2,) + copies.shape[1:])
    copies = lax.all_to_all(copies, ("x", "y"), 0, 0, tiled=True)
    rows, correlation = finish_call(place, copies, stack, scale.reshape(1))
    rows = rows.reshape(filtered.shape)
    basis = spread_call(place, exchange([rows[k] for k in range(columns)], columns))
    return (basis, correlation.T)


def solution(mesh):
    slabs = mesh.shape["slab"]
    columns = mesh.shape["probe"]
    side = math.isqrt(slabs // 2)
    wide = Mesh(mesh.devices.reshape(side, side, 2, columns), ("x", "y", "core", "probe"))
    slab = ("x", "y", "core")
    in_specs = (
        P("probe", None, slab, None, None),
        P(None, None, slab, "probe", None),
        P(slab, None, None),
        P(None, slab, None, None),
    )
    out_specs = (P("probe", None, slab, None, None), P())

    def step(probes, earlier, modulus, tangent):
        length = math.prod(probes.shape[1:])
        scale = jnp.sqrt(jnp.float32(length))
        inner = lambda *parts: body(*parts, slabs, columns, scale)
        return jax.shard_map(inner, mesh=wide, in_specs=in_specs, out_specs=out_specs, check_vma=False)(
            probes, earlier, modulus, tangent
        )

    return step
```

```python
import functools
import math

import jax
import jax.numpy as jnp
from jax import lax
from jax.experimental import pallas as pl
from jax.experimental.pallas import tpu as pltpu
from jax.sharding import Mesh
from jax.sharding import PartitionSpec as P

STRIP = 16
PART = 0.05 / 16.0


def rows_at(ref, lead, start, shift, height):
    first = start + shift
    if first < 0:
        block = pltpu.roll(ref[lead + (pl.ds(0, STRIP), slice(None))], 1, 0)
        row = lax.broadcasted_iota(jnp.int32, block.shape, 0)
        return jnp.where(row == 0, 0.0, block)
    if first + STRIP > height:
        block = pltpu.roll(ref[lead + (pl.ds(height - STRIP, STRIP), slice(None))], STRIP - 1, 0)
        row = lax.broadcasted_iota(jnp.int32, block.shape, 0)
        return jnp.where(row == STRIP - 1, 0.0, block)
    return ref[lead + (pl.ds(first, STRIP), slice(None))]


def across(block):
    breadth = block.shape[1]
    lane = lax.broadcasted_iota(jnp.int32, block.shape, 1)
    left = jnp.where(lane == 0, 0.0, pltpu.roll(block, 1, 1))
    right = jnp.where(lane == breadth - 1, 0.0, pltpu.roll(block, breadth - 1, 1))
    return left + right


def outer_sum(mid, above, below):
    tall = (mid + mid) + (above + below)
    both = tall + mid
    return across(tall) + (both + both)


def full_sum(mid, pair_y, side, side_y):
    near = pair_y + side
    six = 6.0 * mid
    inner = (near + near) + (six + side_y)
    rest = inner + (near - six)
    return across(inner) + (rest + rest)


def combine(diag, off, fields):
    a, b, c = fields
    return (
        diag[0] * a + off[0] * b + off[1] * c,
        off[0] * a + diag[1] * b + off[2] * c,
        off[1] * a + off[2] * b + diag[2] * c,
    )


def lift_kernel(place, probes_far, modulus_far, out, sems):
    count = probes_far.shape[0]
    core = place[0]
    copies = [
        pltpu.make_async_copy(probes_far.at[k, :, core], out.at[pl.ds(3 * k, 3)], sems.at[k]) for k in range(count)
    ]
    copies.append(pltpu.make_async_copy(modulus_far.at[pl.ds(core, 1)], out.at[pl.ds(3 * count, 1)], sems.at[count]))
    for copy in copies:
        copy.start()
    for copy in copies:
        copy.wait()


def partial_kernel(place, probes_far, modulus_far, tangent_far, far, near, probes, modulus, tangent, prod, sems):
    count = probes.shape[0]
    height = probes.shape[3]
    core = place[0]
    copies = []
    for z, plane in ((0, core), (1, 1 - core)):
        triples = (
            (modulus_far.at[pl.ds(plane, 1)], modulus.at[pl.ds(z, 1)]),
            (probes_far.at[:, :, pl.ds(plane, 1)], probes.at[:, :, pl.ds(z, 1)]),
            (tangent_far.at[:, pl.ds(plane, 1)], tangent.at[:, pl.ds(z, 1)]),
        )
        copies.append([pltpu.make_async_copy(src, dst, sems.at[z, n]) for n, (src, dst) in enumerate(triples)])
    for n in range(3):
        copies[0][n].start()
        copies[1][n].start()
    for n in range(2):
        copies[0][n].wait()
        copies[1][n].wait()
    for z in range(2):
        for k in range(count):
            for i in range(3):
                prod[z * 3 * count + 3 * k + i] = probes[k, i, z] * modulus[z]
    copies[0][2].wait()
    copies[1][2].wait()
    for z, out in ((0, far), (1, near)):
        other = 1 - z
        for s in range(0, height, STRIP):
            here = pl.ds(s, STRIP)

            def mod(plane, shift):
                return rows_at(modulus, (plane,), s, shift, height)

            m = mod(z, 0)
            side = mod(other, 0)
            neighbours = full_sum(m, mod(z, -1) + mod(z, 1), side, mod(other, -1) + mod(other, 1))
            common = (3.4 / 16.0) * m + PART * neighbours - 1.0
            diag = [common + 0.125 * tangent[i, z, here, :] for i in range(3)]
            off = [0.125 * tangent[3 + i, z, here, :] for i in range(3)]
            scaled = PART * m
            if z:
                out[6 * count, here, :] = m
            for k in range(count):
                values = [probes[k, i, z, here, :] for i in range(3)]
                mixed = combine(diag, off, values)
                for i in range(3):
                    def val(plane, shift):
                        return rows_at(probes, (k, i, plane), s, shift, height)

                    def pro(plane, shift):
                        return rows_at(prod, (plane * 3 * count + 3 * k + i,), s, shift, height)

                    first = full_sum(values[i], val(z, -1) + val(z, 1), val(other, 0), val(other, -1) + val(other, 1))
                    second = full_sum(pro(z, 0), pro(z, -1) + pro(z, 1), pro(other, 0), pro(other, -1) + pro(other, 1))
                    if z:
                        out[3 * k + i, here, :] = values[i]
                    out[3 * count * z + 3 * k + i, here, :] = mixed[i] - scaled * first - PART * second


def filter_kernel(place, lo, lo_part, down, down_part, up, hi, tangent_far, out, tangent, once, prod, sums, products, prior, sems):
    planes = (lo, down, up, hi)
    core = place[0]
    parts = (lo_part, down_part, up, hi)
    copies = [
        pltpu.make_async_copy(tangent_far.at[:, pl.ds(plane, 1)], tangent.at[:, pl.ds(z, 1)], sems.at[z])
        for z, plane in ((0, core), (1, 1 - core))
    ]
    for copy in copies:
        copy.start()
    total = lo.shape[0] - 1
    count = total // 3
    height = lo.shape[1]
    blocks = height // STRIP
    last = (total, total, 2 * total, 2 * total)
    start = (0, 0, total, total)
    mods = [planes[z][last[z]] for z in range(4)]
    for z in range(4):
        for n in range(total):
            prior[z * total + n] = planes[z][n] * mods[z]
    for source, target in ((0, 1), (1, 0), (2, 3), (3, 2)):
        src = planes[source]
        dst = planes[target]
        for s in range(0, height, STRIP):
            here = pl.ds(s, STRIP)

            def at(ref, n, shift):
                return rows_at(ref, (n,), s, shift, height)

            m = dst[last[target], here, :]
            weight = PART * outer_sum(*(at(src, last[source], d) for d in (0, -1, 1)))
            scaled = PART * m
            for n in range(total):
                first = outer_sum(at(src, n, 0), at(src, n, -1), at(src, n, 1))
                j = source * total + n
                second = outer_sum(at(prior, j, 0), at(prior, j, -1), at(prior, j, 1))
                value = parts[target][start[target] + n, here, :] + weight * dst[n, here, :] - scaled * first - PART * second
                if target in (0, 3):
                    value = jnp.where(m > 0.0, value, 0.0)
                once[target * total + n, here, :] = value
                prod[target * total + n, here, :] = value * m
    for z in (1, 2):
        for n in range(total):
            sums[(z - 1) * total + n] = once[(z - 1) * total + n] + once[(z + 1) * total + n]
            products[(z - 1) * total + n] = prod[(z - 1) * total + n] + prod[(z + 1) * total + n]
    for copy in copies:
        copy.wait()
    for z, depth in ((1, core), (2, 1 - core)):
        plane = planes[z]
        for s in range(0, height, STRIP):
            here = pl.ds(s, STRIP)

            def at(ref, n, shift):
                return rows_at(ref, (n,), s, shift, height)

            def mod(p, shift):
                return rows_at(planes[p], (last[p],), s, shift, height)

            m = mod(z, 0)
            side = [mod(z - 1, d) + mod(z + 1, d) for d in (-1, 0, 1)]
            neighbours = full_sum(m, mod(z, -1) + mod(z, 1), side[1], side[0] + side[2])
            common = (6.8 / 16.0) * m + (2.0 * PART) * neighbours - 2.0
            diag = [common + 0.25 * tangent[i, z - 1, here, :] for i in range(3)]
            off = [0.25 * tangent[3 + i, z - 1, here, :] for i in range(3)]
            scaled = (2.0 * PART) * m
            turn = lax.rem(s // STRIP + blocks - place[1], blocks)
            for k in range(count):
                base = z * total + 3 * k
                mixed = combine(diag, off, [once[base + i, here, :] for i in range(3)])
                for i in range(3):
                    n = base + i
                    j = n - total
                    first = full_sum(at(once, n, 0), at(once, n, -1) + at(once, n, 1), at(sums, j, 0), at(sums, j, -1) + at(sums, j, 1))
                    second = full_sum(at(prod, n, 0), at(prod, n, -1) + at(prod, n, 1), at(products, j, 0), at(products, j, -1) + at(products, j, 1))
                    value = mixed[i] - scaled * first - (2.0 * PART) * second - plane[3 * k + i, here, :]
                    out[turn, k, i, depth] = value


def split(block):
    high = block.astype(jnp.bfloat16).astype(jnp.float32)
    rest = block - high
    middle = rest.astype(jnp.bfloat16).astype(jnp.float32)
    return high, middle, rest - middle


def piled(block):
    parts = list(split(block))
    if block.shape[0] % 16:
        parts.append(jnp.zeros_like(block))
    return jnp.concatenate(parts, axis=0).astype(jnp.bfloat16)


def folded(block, count, start, axis):
    pieces = [lax.slice_in_dim(block, start + n * count, start + (n + 1) * count, axis=axis) for n in range(3)]
    return (pieces[0] + pieces[1]) + pieces[2]


WIDE = 8


def gram_kernel(place, *refs, pieces, alone):
    stack, out, tall = refs[-3:]
    chunks = refs[: len(pieces)]
    earlier = refs[len(pieces) : -3]
    length = stack.shape[0]
    count = tall.shape[0] // length
    for chunk, (turn, first) in zip(chunks, pieces):
        each = chunk.shape[0]
        base = first
        if not alone:
            source = place[1] - turn
            base = first + 2 * jnp.where(source < 0, source + count // 2, source)
        for j in range(each):
            tall[pl.ds(base + j, length, stride=count), :] = chunk[j]

    def step(r, gram):
        rows = []
        for h in range(WIDE):
            here = WIDE * r + h
            pile = piled(tall[pl.ds(here * count, count), :])
            stack[here] = pile
            rows.append(pile)
        own = jnp.concatenate(rows, axis=1)
        others = [jnp.concatenate([e[WIDE * r + h] for h in range(WIDE)], axis=1) for e in earlier]
        every = jnp.concatenate(others + [own], axis=0)
        return gram + lax.dot_general(own, every, (((1,), (1,)), ((), ())), preferred_element_type=jnp.float32)

    width = 3 * count * (1 + len(earlier))
    gram = lax.fori_loop(0, length // WIDE, step, jnp.zeros((3 * count, width), jnp.float32), unroll=2)
    gram = folded(gram, count, 0, 0)
    found = [folded(gram, count, 3 * count * n, 1) for n in range(1 + len(earlier))]
    if alone:
        found.append(jnp.zeros((count, count), jnp.float32))
    out[...] = jnp.concatenate(found, axis=1)


def pack_kernel(first, second, out):
    gram = jnp.concatenate([first[...], second[...]], axis=0)
    packed = jnp.concatenate([gram[8 * q : 8 * q + 8] for q in range(gram.shape[0] // 8)], axis=1)
    for n in range(out.shape[0]):
        out[n] = packed


def finish_kernel(place, copies, first, second, scale, out, correlation):
    length = first.shape[0]
    kept = first.shape[1] // 3
    made = second.shape[1] // 3
    total = kept + made
    summed = copies[0]
    for n in range(1, copies.shape[0]):
        summed = summed + copies[n]
    gram = jnp.concatenate([summed[:, total * q : total * q + total] for q in range(total // 8)], axis=0)
    row = lax.broadcasted_iota(jnp.int32, (total, total), 0)
    column = lax.broadcasted_iota(jnp.int32, (total, total), 1)
    unit = jnp.where(row == column, 1.0, 0.0)
    strict = jnp.where(row > column, gram, 0.0)
    mirrored = lax.dot_general(strict, unit, (((0,), (0,)), ((), ())), precision=lax.Precision.HIGHEST)
    gram = jnp.where(row >= column, gram, mirrored)
    work = jnp.concatenate([gram, unit, jnp.zeros((total, 128 - 2 * total), jnp.float32)], axis=1)
    slot = lax.broadcasted_iota(jnp.int32, (total, 1), 0)
    pivots = jnp.zeros((total, 1), jnp.float32)
    factor = scale[0]
    for k in range(total):
        if k == kept:
            correlation[...] = -factor * work[kept:, total : total + kept]
        pivot = work[k : k + 1, k : k + 1]
        ratio = jnp.where(slot > k, work[:, k : k + 1] / pivot, 0.0)
        pivots = jnp.where(slot == k, pivot, pivots)
        work = work - ratio * work[k : k + 1, :]
    weights = factor * work[kept:, total : 2 * total] * lax.rsqrt(pivots[kept:])
    there = lax.broadcasted_iota(jnp.int32, (made, made), 0)
    source = lax.broadcasted_iota(jnp.int32, (made, made), 1)
    moved = there + 2 * place[1]
    turn = jnp.where(jnp.where(moved >= made, moved - made, moved) == source, 1.0, 0.0)
    weights = jnp.dot(turn, weights, precision=lax.Precision.HIGHEST)
    lines = []
    for part in split(weights):
        lines.append(jnp.concatenate([part[:, :kept]] * 3 + [part[:, kept:]] * 3, axis=1))
    left = jnp.concatenate(lines, axis=0).astype(jnp.bfloat16)
    for r in range(0, length, 2):
        sides = [jnp.concatenate([first[r + h], second[r + h]], axis=0) for h in range(2)]
        both = jnp.concatenate(sides, axis=1)
        wide_rows = lax.dot_general(left, both, (((1,), (0,)), ((), ())), preferred_element_type=jnp.float32)
        rows = (wide_rows[:made] + wide_rows[made : 2 * made]) + wide_rows[2 * made :]
        for h in range(2):
            out[pl.ds(r + h, made, stride=length), :] = rows[:, 128 * h : 128 * h + 128]


def out_turns(blocks):
    half = (len(blocks) - 1) // 2
    listed = []
    for n, block in enumerate(blocks):
        turn = n if n <= half else n - 1
        listed.append((block, turn, blocks[half].shape[0] if n == half + 1 else 0))
    return listed


def spread_kernel(place, *refs):
    blocks, out, sems = refs[:-2], refs[-2], refs[-1]
    turns = len(blocks) - 1
    copies = []
    for n, (block, k, first) in enumerate(out_turns(blocks)):
        source = lax.rem(place[1] + turns - k, turns)
        target = out.at[pl.ds(first, block.shape[0]), :, :, pl.ds(source * STRIP, STRIP), :]
        copies.append(pltpu.make_async_copy(block, target, sems.at[n]))
    for copy in copies:
        copy.start()
    for copy in copies:
        copy.wait()


VM = pl.BlockSpec(memory_space=pltpu.VMEM)
SM = pl.BlockSpec(memory_space=pltpu.SMEM)
FAR = pl.BlockSpec(memory_space=pltpu.HBM)


def near_chip(*arrays):
    return tuple(pltpu.with_memory_space_constraint(a, pltpu.VMEM) for a in arrays)


def in_far(*arrays):
    return tuple(pltpu.with_memory_space_constraint(a, pltpu.HBM) for a in arrays)


def lift_call(place, probes, modulus):
    count, _, _, height, breadth = probes.shape
    return pl.pallas_call(
        lift_kernel,
        out_shape=pltpu.VMEM((3 * count + 1, height, breadth), jnp.float32),
        in_specs=[SM, FAR, FAR],
        out_specs=VM,
        scratch_shapes=[pltpu.SemaphoreType.DMA((count + 1,))],
        compiler_params=pltpu.CompilerParams(vmem_limit_bytes=1 << 20),
        name="lift",
    )(place, *in_far(probes, modulus))


def partial_call(place, probes, modulus, tangent):
    count, _, _, height, breadth = probes.shape
    plane = lambda n: pltpu.VMEM((n, height, breadth), jnp.float32)
    return pl.pallas_call(
        partial_kernel,
        out_shape=(plane(3 * count), plane(6 * count + 1)),
        in_specs=[SM] + [FAR] * 3,
        out_specs=(VM, VM),
        scratch_shapes=[pltpu.VMEM(a.shape, jnp.float32) for a in (probes, modulus, tangent)]
        + [plane(6 * count), pltpu.SemaphoreType.DMA((2, 3))],
        compiler_params=pltpu.CompilerParams(vmem_limit_bytes=12 << 20),
        name="partial",
    )(place, *in_far(probes, modulus, tangent))


def filter_call(place, packs, tangent):
    packed, height, breadth = packs[0].shape
    total = packed - 1
    plane = lambda n: pltpu.VMEM((n, height, breadth), jnp.float32)
    return pl.pallas_call(
        filter_kernel,
        out_shape=pltpu.VMEM((height // STRIP, total // 3, 3, 2, STRIP, breadth), jnp.float32),
        in_specs=[SM] + [VM] * len(packs) + [FAR],
        out_specs=VM,
        scratch_shapes=[pltpu.VMEM(tangent.shape, jnp.float32), plane(4 * total), plane(4 * total)]
        + [plane(2 * total), plane(2 * total), plane(4 * total), pltpu.SemaphoreType.DMA((2,))],
        compiler_params=pltpu.CompilerParams(vmem_limit_bytes=16 << 20),
        name="filter",
    )(place, *near_chip(*packs), *in_far(tangent))


def gram_call(place, chunks, pieces, earlier=()):
    alone = not earlier
    length, breadth = chunks[0].shape[1:]
    count = sum(c.shape[0] for c in chunks)
    return pl.pallas_call(
        functools.partial(gram_kernel, pieces=pieces, alone=alone),
        out_shape=(
            pltpu.VMEM((length, 3 * count, breadth), jnp.bfloat16),
            pltpu.VMEM((count, 2 * count), jnp.float32),
        ),
        in_specs=[SM] + [VM] * (len(chunks) + len(earlier)),
        out_specs=(VM, VM),
        scratch_shapes=[pltpu.VMEM((length * count, breadth), jnp.float32)],
        compiler_params=pltpu.CompilerParams(vmem_limit_bytes=8 << 20),
        name="gram",
    )(place, *near_chip(*chunks, *earlier))


def pack_call(grams, copies):
    total = grams[0].shape[1]
    return pl.pallas_call(
        pack_kernel,
        out_shape=pltpu.VMEM((copies, 8, total * total // 8), jnp.float32),
        in_specs=[VM] * 2,
        out_specs=VM,
        compiler_params=pltpu.CompilerParams(vmem_limit_bytes=4 << 20),
        name="pack",
    )(*near_chip(*grams))


def finish_call(place, copies, stacks, scale):
    length, _, breadth = stacks[0].shape
    return pl.pallas_call(
        finish_kernel,
        out_shape=(
            pltpu.VMEM((16 * length, breadth), jnp.float32),
            jax.ShapeDtypeStruct((16, 16), jnp.float32),
        ),
        in_specs=[SM] + [VM] * 3 + [SM],
        out_specs=(VM, VM),
        compiler_params=pltpu.CompilerParams(vmem_limit_bytes=8 << 20),
        name="finish",
    )(place, *near_chip(copies, *stacks), scale)


def spread_call(place, blocks):
    count, parts, depth, strip, breadth = blocks[0].shape
    return pl.pallas_call(
        spread_kernel,
        out_shape=jax.ShapeDtypeStruct((count, parts, depth, strip * (len(blocks) - 1), breadth), jnp.float32),
        in_specs=[SM] + [VM] * len(blocks),
        out_specs=FAR,
        scratch_shapes=[pltpu.SemaphoreType.DMA((len(blocks),))],
        compiler_params=pltpu.CompilerParams(vmem_limit_bytes=8 << 20),
        name="spread",
    )(place, *near_chip(*blocks))


def shift(block, by, columns):
    return lax.ppermute(block, "probe", [(j, (j + by) % columns) for j in range(columns)])


def exchange(parts, columns):
    half = columns // 2
    cut = parts[half].shape[0] // 2
    got = [parts[0]] + [None] * (columns - 1)
    ahead = shift(parts[half][:cut], half, columns)
    back = shift(parts[half][cut:], -(half // 2), columns)
    for k in range(1, columns):
        if k != half:
            got[k] = shift(parts[k], k, columns)
    back = shift(back, half // 2 - half, columns)
    return got[:half] + [ahead, back] + got[half + 1 :]


def body(probes, earlier, modulus, tangent, slabs, columns, scale):
    kept = earlier.shape[0]
    breadth = earlier.shape[-1]
    length = math.prod(earlier.shape[1:-1])
    place = jnp.stack([lax.axis_index("core"), lax.axis_index("probe")]).astype(jnp.int32)
    places = ("x", "y", "core")
    outer = [(i, i + 1) for i in range(1, slabs - 1, 2)] + [(i, i - 1) for i in range(2, slabs, 2)]
    raw = lift_call(place, probes, modulus)
    got_raw = lax.ppermute(raw, places, outer)
    far, near = partial_call(place, probes, modulus, tangent)
    got_far = lax.ppermute(far, places, outer)
    got_near = lax.ppermute(near, "core", [(0, 1), (1, 0)])
    first, first_gram = gram_call(place, [earlier.reshape(kept, length, breadth)], ((0, 0),))
    filtered = filter_call(place, (got_raw, got_far, raw, far, near, got_near), tangent)
    got = exchange([filtered[k] for k in range(columns)], columns)
    half = columns // 2
    pieces = [(k, 0) for k in range(half + 1)] + [(half, 1)] + [(k, 0) for k in range(half + 1, columns)]
    flat = [g.reshape(g.shape[0], length, breadth) for g in got]
    second, second_gram = gram_call(place, flat, tuple(pieces), (first,))
    copies = pack_call((first_gram, second_gram), 2 * columns)
    copies = lax.all_to_all(copies, ("probe", "core"), 0, 0, tiled=True)
    copies = jnp.broadcast_to(jnp.sum(copies, axis=0, keepdims=True), (slabs // 2,) + copies.shape[1:])
    copies = lax.all_to_all(copies, ("x", "y"), 0, 0, tiled=True)
    rows, correlation = finish_call(place, copies, (first, second), scale.reshape(1))
    rows = rows.reshape((columns, 2) + earlier.shape[1:])
    got = exchange([rows[k] for k in range(columns)], columns)
    basis = spread_call(place, got)
    return (basis, correlation.T)


def solution(mesh):
    slabs = mesh.shape["slab"]
    columns = mesh.shape["probe"]
    side = math.isqrt(slabs // 2)
    wide = Mesh(mesh.devices.reshape(side, side, 2, columns), ("x", "y", "core", "probe"))
    slab = ("x", "y", "core")
    in_specs = (
        P("probe", None, slab, None, None),
        P(None, None, slab, "probe", None),
        P(slab, None, None),
        P(None, slab, None, None),
    )
    out_specs = (P("probe", None, slab, None, None), P())

    def step(probes, earlier, modulus, tangent):
        length = math.prod(probes.shape[1:])
        scale = jnp.sqrt(jnp.float32(length))
        inner = lambda *parts: body(*parts, slabs, columns, scale)
        return jax.shard_map(inner, mesh=wide, in_specs=in_specs, out_specs=out_specs, check_vma=False)(
            probes, earlier, modulus, tangent
        )

    return step
```

```python
import functools
import math

import jax
import jax.numpy as jnp
from jax import lax
from jax.experimental import pallas as pl
from jax.experimental.pallas import tpu as pltpu
from jax.sharding import Mesh
from jax.sharding import PartitionSpec as P

STRIP = 16
PART = 0.05 / 16.0


def rows_at(ref, lead, start, shift, height):
    first = start + shift
    if first < 0:
        block = pltpu.roll(ref[lead + (pl.ds(0, STRIP), slice(None))], 1, 0)
        row = lax.broadcasted_iota(jnp.int32, block.shape, 0)
        return jnp.where(row == 0, 0.0, block)
    if first + STRIP > height:
        block = pltpu.roll(ref[lead + (pl.ds(height - STRIP, STRIP), slice(None))], STRIP - 1, 0)
        row = lax.broadcasted_iota(jnp.int32, block.shape, 0)
        return jnp.where(row == STRIP - 1, 0.0, block)
    return ref[lead + (pl.ds(first, STRIP), slice(None))]


def across(block):
    breadth = block.shape[1]
    lane = lax.broadcasted_iota(jnp.int32, block.shape, 1)
    left = jnp.where(lane == 0, 0.0, pltpu.roll(block, 1, 1))
    right = jnp.where(lane == breadth - 1, 0.0, pltpu.roll(block, breadth - 1, 1))
    return left + right


def outer_sum(mid, above, below):
    tall = (mid + mid) + (above + below)
    both = tall + mid
    return across(tall) + (both + both)


def full_sum(mid, pair_y, side, side_y):
    near = pair_y + side
    six = 6.0 * mid
    inner = (near + near) + (six + side_y)
    rest = inner + (near - six)
    return across(inner) + (rest + rest)


def combine(diag, off, fields):
    a, b, c = fields
    return (
        diag[0] * a + off[0] * b + off[1] * c,
        off[0] * a + diag[1] * b + off[2] * c,
        off[1] * a + off[2] * b + diag[2] * c,
    )


def lift_kernel(probes_far, modulus_far, out, sems):
    count = probes_far.shape[0]
    core = lax.axis_index("core")
    copies = [
        pltpu.make_async_copy(probes_far.at[k, :, core], out.at[pl.ds(3 * k, 3)], sems.at[k]) for k in range(count)
    ]
    copies.append(pltpu.make_async_copy(modulus_far.at[pl.ds(core, 1)], out.at[pl.ds(3 * count, 1)], sems.at[count]))
    for copy in copies:
        copy.start()
    for copy in copies:
        copy.wait()


def partial_kernel(probes, modulus, tangent, far, near, prod):
    count = probes.shape[0]
    height = probes.shape[3]
    core = lax.axis_index("core")
    depth = (core, 1 - core)
    for z in range(2):
        for k in range(count):
            for i in range(3):
                prod[z * 3 * count + 3 * k + i] = probes[k, i, depth[z]] * modulus[depth[z]]
    for z, out in ((0, far), (1, near)):
        other = 1 - z
        for s in range(0, height, STRIP):
            here = pl.ds(s, STRIP)

            def mod(plane, shift):
                return rows_at(modulus, (depth[plane],), s, shift, height)

            m = mod(z, 0)
            side = mod(other, 0)
            neighbours = full_sum(m, mod(z, -1) + mod(z, 1), side, mod(other, -1) + mod(other, 1))
            common = (3.4 / 16.0) * m + PART * neighbours - 1.0
            diag = [common + 0.125 * tangent[i, depth[z], here, :] for i in range(3)]
            off = [0.125 * tangent[3 + i, depth[z], here, :] for i in range(3)]
            scaled = PART * m
            if z:
                out[6 * count, here, :] = m
            for k in range(count):
                values = [probes[k, i, depth[z], here, :] for i in range(3)]
                mixed = combine(diag, off, values)
                for i in range(3):
                    def val(plane, shift):
                        return rows_at(probes, (k, i, depth[plane]), s, shift, height)

                    def pro(plane, shift):
                        return rows_at(prod, (plane * 3 * count + 3 * k + i,), s, shift, height)

                    first = full_sum(values[i], val(z, -1) + val(z, 1), val(other, 0), val(other, -1) + val(other, 1))
                    second = full_sum(pro(z, 0), pro(z, -1) + pro(z, 1), pro(other, 0), pro(other, -1) + pro(other, 1))
                    if z:
                        out[3 * k + i, here, :] = values[i]
                    out[3 * count * z + 3 * k + i, here, :] = mixed[i] - scaled * first - PART * second


def filter_kernel(lo, lo_part, down, down_part, up, hi, tangent, out, once, prod, sums, products, prior):
    planes = (lo, down, up, hi)
    core = lax.axis_index("core")
    parts = (lo_part, down_part, up, hi)
    total = lo.shape[0] - 1
    count = total // 3
    height = lo.shape[1]
    blocks = height // STRIP
    last = (total, total, 2 * total, 2 * total)
    start = (0, 0, total, total)
    for z in range(4):
        for n in range(total):
            prior[z * total + n] = planes[z][n] * planes[z][last[z]]
    for source, target in ((0, 1), (1, 0), (2, 3), (3, 2)):
        src = planes[source]
        dst = planes[target]
        for s in range(0, height, STRIP):
            here = pl.ds(s, STRIP)

            def at(ref, n, shift):
                return rows_at(ref, (n,), s, shift, height)

            m = dst[last[target], here, :]
            weight = PART * outer_sum(*(at(src, last[source], d) for d in (0, -1, 1)))
            scaled = PART * m
            for n in range(total):
                first = outer_sum(at(src, n, 0), at(src, n, -1), at(src, n, 1))
                j = source * total + n
                second = outer_sum(at(prior, j, 0), at(prior, j, -1), at(prior, j, 1))
                value = parts[target][start[target] + n, here, :] + weight * dst[n, here, :] - scaled * first - PART * second
                if target in (0, 3):
                    value = jnp.where(m > 0.0, value, 0.0)
                once[target * total + n, here, :] = value
                prod[target * total + n, here, :] = value * m
    for z in (1, 2):
        for n in range(total):
            sums[(z - 1) * total + n] = once[(z - 1) * total + n] + once[(z + 1) * total + n]
            products[(z - 1) * total + n] = prod[(z - 1) * total + n] + prod[(z + 1) * total + n]
    for z, depth in ((1, core), (2, 1 - core)):
        plane = planes[z]
        for s in range(0, height, STRIP):
            here = pl.ds(s, STRIP)

            def at(ref, n, shift):
                return rows_at(ref, (n,), s, shift, height)

            def mod(p, shift):
                return rows_at(planes[p], (last[p],), s, shift, height)

            m = mod(z, 0)
            side = [mod(z - 1, d) + mod(z + 1, d) for d in (-1, 0, 1)]
            neighbours = full_sum(m, mod(z, -1) + mod(z, 1), side[1], side[0] + side[2])
            common = (6.8 / 16.0) * m + (2.0 * PART) * neighbours - 2.0
            diag = [common + 0.25 * tangent[i, depth, here, :] for i in range(3)]
            off = [0.25 * tangent[3 + i, depth, here, :] for i in range(3)]
            scaled = (2.0 * PART) * m
            turn = lax.rem(s // STRIP + blocks - lax.axis_index("probe"), blocks)
            for k in range(count):
                base = z * total + 3 * k
                mixed = combine(diag, off, [once[base + i, here, :] for i in range(3)])
                for i in range(3):
                    n = base + i
                    j = n - total
                    first = full_sum(at(once, n, 0), at(once, n, -1) + at(once, n, 1), at(sums, j, 0), at(sums, j, -1) + at(sums, j, 1))
                    second = full_sum(at(prod, n, 0), at(prod, n, -1) + at(prod, n, 1), at(products, j, 0), at(products, j, -1) + at(products, j, 1))
                    value = mixed[i] - scaled * first - (2.0 * PART) * second - plane[3 * k + i, here, :]
                    out[turn, k, i, depth] = value


def split(block):
    high = block.astype(jnp.bfloat16).astype(jnp.float32)
    rest = block - high
    middle = rest.astype(jnp.bfloat16).astype(jnp.float32)
    return high, middle, rest - middle


def piled(block):
    parts = list(split(block))
    if block.shape[0] % 16:
        parts.append(jnp.zeros_like(block))
    return jnp.concatenate(parts, axis=0).astype(jnp.bfloat16)


def folded(block, count, start, axis):
    pieces = [lax.slice_in_dim(block, start + n * count, start + (n + 1) * count, axis=axis) for n in range(3)]
    return (pieces[0] + pieces[1]) + pieces[2]


WIDE = 8


def gram_kernel(*refs, pieces, alone):
    stack, out, tall = refs[-3:]
    chunks = refs[: len(pieces)]
    earlier = refs[len(pieces) : -3]
    length = stack.shape[0]
    count = tall.shape[0] // length
    for chunk, (turn, first) in zip(chunks, pieces):
        each = chunk.shape[0]
        base = first
        if not alone:
            source = lax.axis_index("probe") - turn
            base = first + 2 * jnp.where(source < 0, source + count // 2, source)
        for j in range(each):
            tall[pl.ds(base + j, length, stride=count), :] = chunk[j]

    def step(r, gram):
        rows = []
        for h in range(WIDE):
            here = WIDE * r + h
            pile = piled(tall[pl.ds(here * count, count), :])
            stack[here] = pile
            rows.append(pile)
        own = jnp.concatenate(rows, axis=1)
        others = [jnp.concatenate([e[WIDE * r + h] for h in range(WIDE)], axis=1) for e in earlier]
        every = jnp.concatenate(others + [own], axis=0)
        return gram + lax.dot_general(own, every, (((1,), (1,)), ((), ())), preferred_element_type=jnp.float32)

    width = 3 * count * (1 + len(earlier))
    gram = lax.fori_loop(0, length // WIDE, step, jnp.zeros((3 * count, width), jnp.float32), unroll=2)
    gram = folded(gram, count, 0, 0)
    found = [folded(gram, count, 3 * count * n, 1) for n in range(1 + len(earlier))]
    if alone:
        found.append(jnp.zeros((count, count), jnp.float32))
    out[...] = jnp.concatenate(found, axis=1)


def pack_kernel(first, second, out):
    gram = jnp.concatenate([first[...], second[...]], axis=0)
    packed = jnp.concatenate([gram[8 * q : 8 * q + 8] for q in range(gram.shape[0] // 8)], axis=1)
    for n in range(out.shape[0]):
        out[n] = packed


def finish_kernel(copies, first, second, out, correlation, *, factor):
    length = first.shape[0]
    kept = first.shape[1] // 3
    made = second.shape[1] // 3
    total = kept + made
    summed = copies[0]
    for n in range(1, copies.shape[0]):
        summed = summed + copies[n]
    gram = jnp.concatenate([summed[:, total * q : total * q + total] for q in range(total // 8)], axis=0)
    row = lax.broadcasted_iota(jnp.int32, (total, total), 0)
    column = lax.broadcasted_iota(jnp.int32, (total, total), 1)
    unit = jnp.where(row == column, 1.0, 0.0)
    strict = jnp.where(row > column, gram, 0.0)
    mirrored = lax.dot_general(strict, unit, (((0,), (0,)), ((), ())), precision=lax.Precision.HIGHEST)
    gram = jnp.where(row >= column, gram, mirrored)
    work = jnp.concatenate([gram, unit, jnp.zeros((total, 128 - 2 * total), jnp.float32)], axis=1)
    slot = lax.broadcasted_iota(jnp.int32, (total, 1), 0)
    pivots = jnp.zeros((total, 1), jnp.float32)
    for k in range(total):
        if k == kept:
            correlation[...] = -factor * work[kept:, total : total + kept]
        pivot = work[k : k + 1, k : k + 1]
        ratio = jnp.where(slot > k, work[:, k : k + 1] / pivot, 0.0)
        pivots = jnp.where(slot == k, pivot, pivots)
        work = work - ratio * work[k : k + 1, :]
    weights = factor * work[kept:, total : 2 * total] * lax.rsqrt(pivots[kept:])
    there = lax.broadcasted_iota(jnp.int32, (made, made), 0)
    source = lax.broadcasted_iota(jnp.int32, (made, made), 1)
    moved = there + 2 * lax.axis_index("probe")
    turn = jnp.where(jnp.where(moved >= made, moved - made, moved) == source, 1.0, 0.0)
    weights = jnp.dot(turn, weights, precision=lax.Precision.HIGHEST)
    lines = []
    for part in split(weights):
        lines.append(jnp.concatenate([part[:, :kept]] * 3 + [part[:, kept:]] * 3, axis=1))
    left = jnp.concatenate(lines, axis=0).astype(jnp.bfloat16)
    for r in range(0, length, 2):
        sides = [jnp.concatenate([first[r + h], second[r + h]], axis=0) for h in range(2)]
        both = jnp.concatenate(sides, axis=1)
        wide_rows = lax.dot_general(left, both, (((1,), (0,)), ((), ())), preferred_element_type=jnp.float32)
        rows = (wide_rows[:made] + wide_rows[made : 2 * made]) + wide_rows[2 * made :]
        for h in range(2):
            out[pl.ds(r + h, made, stride=length), :] = rows[:, 128 * h : 128 * h + 128]


def out_turns(blocks):
    half = (len(blocks) - 1) // 2
    listed = []
    for n, block in enumerate(blocks):
        turn = n if n <= half else n - 1
        listed.append((block, turn, blocks[half].shape[0] if n == half + 1 else 0))
    return listed


def spread_kernel(*refs):
    blocks, out, sems = refs[:-2], refs[-2], refs[-1]
    turns = len(blocks) - 1
    copies = []
    for n, (block, k, first) in enumerate(out_turns(blocks)):
        source = lax.rem(lax.axis_index("probe") + turns - k, turns)
        target = out.at[pl.ds(first, block.shape[0]), :, :, pl.ds(source * STRIP, STRIP), :]
        copies.append(pltpu.make_async_copy(block, target, sems.at[n]))
    for copy in copies:
        copy.start()
    for copy in copies:
        copy.wait()


VM = pl.BlockSpec(memory_space=pltpu.VMEM)
FAR = pl.BlockSpec(memory_space=pltpu.HBM)


def near_chip(*arrays):
    return tuple(pltpu.with_memory_space_constraint(a, pltpu.VMEM) for a in arrays)


def in_far(*arrays):
    return tuple(pltpu.with_memory_space_constraint(a, pltpu.HBM) for a in arrays)


def lift_call(probes, modulus):
    count, _, _, height, breadth = probes.shape
    return pl.pallas_call(
        lift_kernel,
        out_shape=pltpu.VMEM((3 * count + 1, height, breadth), jnp.float32),
        in_specs=[FAR, FAR],
        out_specs=VM,
        scratch_shapes=[pltpu.SemaphoreType.DMA((count + 1,))],
        compiler_params=pltpu.CompilerParams(vmem_limit_bytes=1 << 20),
        name="lift",
    )(*in_far(probes, modulus))


def partial_call(probes, modulus, tangent):
    count, _, _, height, breadth = probes.shape
    plane = lambda n: pltpu.VMEM((n, height, breadth), jnp.float32)
    return pl.pallas_call(
        partial_kernel,
        out_shape=(plane(3 * count), plane(6 * count + 1)),
        in_specs=[VM] * 3,
        out_specs=(VM, VM),
        scratch_shapes=[plane(6 * count)],
        compiler_params=pltpu.CompilerParams(vmem_limit_bytes=12 << 20),
        name="partial",
    )(*near_chip(probes, modulus, tangent))


def filter_call(packs, tangent):
    packed, height, breadth = packs[0].shape
    total = packed - 1
    plane = lambda n: pltpu.VMEM((n, height, breadth), jnp.float32)
    return pl.pallas_call(
        filter_kernel,
        out_shape=pltpu.VMEM((height // STRIP, total // 3, 3, 2, STRIP, breadth), jnp.float32),
        in_specs=[VM] * (len(packs) + 1),
        out_specs=VM,
        scratch_shapes=[plane(n * total) for n in (4, 4, 2, 2, 4)],
        compiler_params=pltpu.CompilerParams(vmem_limit_bytes=16 << 20),
        name="filter",
    )(*near_chip(*packs, tangent))


def gram_call(chunks, pieces, earlier=()):
    alone = not earlier
    length, breadth = chunks[0].shape[1:]
    count = sum(c.shape[0] for c in chunks)
    return pl.pallas_call(
        functools.partial(gram_kernel, pieces=pieces, alone=alone),
        out_shape=(
            pltpu.VMEM((length, 3 * count, breadth), jnp.bfloat16),
            pltpu.VMEM((count, 2 * count), jnp.float32),
        ),
        in_specs=[VM] * (len(chunks) + len(earlier)),
        out_specs=(VM, VM),
        scratch_shapes=[pltpu.VMEM((length * count, breadth), jnp.float32)],
        compiler_params=pltpu.CompilerParams(vmem_limit_bytes=8 << 20),
        name="gram",
    )(*near_chip(*chunks, *earlier))


def pack_call(grams, copies):
    total = grams[0].shape[1]
    return pl.pallas_call(
        pack_kernel,
        out_shape=pltpu.VMEM((copies, 8, total * total // 8), jnp.float32),
        in_specs=[VM] * 2,
        out_specs=VM,
        compiler_params=pltpu.CompilerParams(vmem_limit_bytes=4 << 20),
        name="pack",
    )(*near_chip(*grams))


def finish_call(copies, stacks, scale):
    length, _, breadth = stacks[0].shape
    return pl.pallas_call(
        functools.partial(finish_kernel, factor=scale),
        out_shape=(
            pltpu.VMEM((16 * length, breadth), jnp.float32),
            jax.ShapeDtypeStruct((16, 16), jnp.float32),
        ),
        in_specs=[VM] * 3,
        out_specs=(VM, VM),
        compiler_params=pltpu.CompilerParams(vmem_limit_bytes=8 << 20),
        name="finish",
    )(*near_chip(copies, *stacks))


def spread_call(blocks):
    count, parts, depth, strip, breadth = blocks[0].shape
    return pl.pallas_call(
        spread_kernel,
        out_shape=jax.ShapeDtypeStruct((count, parts, depth, strip * (len(blocks) - 1), breadth), jnp.float32),
        in_specs=[VM] * len(blocks),
        out_specs=FAR,
        scratch_shapes=[pltpu.SemaphoreType.DMA((len(blocks),))],
        compiler_params=pltpu.CompilerParams(vmem_limit_bytes=8 << 20),
        name="spread",
    )(*near_chip(*blocks))


def shift(block, by, columns):
    return lax.ppermute(block, "probe", [(j, (j + by) % columns) for j in range(columns)])


def exchange(parts, columns):
    half = columns // 2
    cut = parts[half].shape[0] // 2
    got = [parts[0]] + [None] * (columns - 1)
    ahead = shift(parts[half][:cut], half, columns)
    back = shift(parts[half][cut:], -(half // 2), columns)
    for k in range(1, columns):
        if k != half:
            got[k] = shift(parts[k], k, columns)
    back = shift(back, half // 2 - half, columns)
    return got[:half] + [ahead, back] + got[half + 1 :]


def body(probes, earlier, modulus, tangent, slabs, columns, scale):
    kept = earlier.shape[0]
    breadth = earlier.shape[-1]
    length = math.prod(earlier.shape[1:-1])
    places = ("x", "y", "core")
    outer = [(i, i + 1) for i in range(1, slabs - 1, 2)] + [(i, i - 1) for i in range(2, slabs, 2)]
    raw = lift_call(probes, modulus)
    got_raw = lax.ppermute(raw, places, outer)
    far, near = partial_call(probes, modulus, tangent)
    got_far = lax.ppermute(far, places, outer)
    got_near = lax.ppermute(near, "core", [(0, 1), (1, 0)])
    first, first_gram = gram_call([earlier.reshape(kept, length, breadth)], ((0, 0),))
    filtered = filter_call((got_raw, got_far, raw, far, near, got_near), tangent)
    got = exchange([filtered[k] for k in range(columns)], columns)
    half = columns // 2
    pieces = [(k, 0) for k in range(half + 1)] + [(half, 1)] + [(k, 0) for k in range(half + 1, columns)]
    flat = [g.reshape(g.shape[0], length, breadth) for g in got]
    second, second_gram = gram_call(flat, tuple(pieces), (first,))
    copies = pack_call((first_gram, second_gram), 2 * columns)
    copies = lax.all_to_all(copies, ("probe", "core"), 0, 0, tiled=True)
    copies = jnp.broadcast_to(jnp.sum(copies, axis=0, keepdims=True), (slabs // 2,) + copies.shape[1:])
    copies = lax.all_to_all(copies, ("x", "y"), 0, 0, tiled=True)
    rows, correlation = finish_call(copies, (first, second), scale)
    rows = rows.reshape((columns, 2) + earlier.shape[1:])
    got = exchange([rows[k] for k in range(columns)], columns)
    basis = spread_call(got)
    return (basis, correlation.T)


def solution(mesh):
    slabs = mesh.shape["slab"]
    columns = mesh.shape["probe"]
    side = math.isqrt(slabs // 2)
    wide = Mesh(mesh.devices.reshape(side, side, 2, columns), ("x", "y", "core", "probe"))
    slab = ("x", "y", "core")
    in_specs = (
        P("probe", None, slab, None, None),
        P(None, None, slab, "probe", None),
        P(slab, None, None),
        P(None, slab, None, None),
    )
    out_specs = (P("probe", None, slab, None, None), P())

    def step(probes, earlier, modulus, tangent):
        length = math.prod(probes.shape[1:])
        scale = math.sqrt(length)
        inner = lambda *parts: body(*parts, slabs, columns, scale)
        return jax.shard_map(inner, mesh=wide, in_specs=in_specs, out_specs=out_specs, check_vma=False)(
            probes, earlier, modulus, tangent
        )

    return step
```

```python
import functools
import math

import jax
import jax.numpy as jnp
from jax import lax
from jax.experimental import pallas as pl
from jax.experimental.pallas import tpu as pltpu
from jax.sharding import Mesh
from jax.sharding import PartitionSpec as P

STRIP = 16
PART = 0.05 / 16.0


def rows_at(ref, lead, start, shift, height):
    first = start + shift
    if first < 0:
        block = pltpu.roll(ref[lead + (pl.ds(0, STRIP), slice(None))], 1, 0)
        row = lax.broadcasted_iota(jnp.int32, block.shape, 0)
        return jnp.where(row == 0, 0.0, block)
    if first + STRIP > height:
        block = pltpu.roll(ref[lead + (pl.ds(height - STRIP, STRIP), slice(None))], STRIP - 1, 0)
        row = lax.broadcasted_iota(jnp.int32, block.shape, 0)
        return jnp.where(row == STRIP - 1, 0.0, block)
    return ref[lead + (pl.ds(first, STRIP), slice(None))]


def across(block):
    breadth = block.shape[1]
    lane = lax.broadcasted_iota(jnp.int32, block.shape, 1)
    left = jnp.where(lane == 0, 0.0, pltpu.roll(block, 1, 1))
    right = jnp.where(lane == breadth - 1, 0.0, pltpu.roll(block, breadth - 1, 1))
    return left + right


def outer_sum(mid, above, below):
    tall = (mid + mid) + (above + below)
    both = tall + mid
    return across(tall) + (both + both)


def full_sum(mid, pair_y, side, side_y):
    near = pair_y + side
    six = 6.0 * mid
    inner = (near + near) + (six + side_y)
    rest = inner + (near - six)
    return across(inner) + (rest + rest)


def combine(diag, off, fields):
    a, b, c = fields
    return (
        diag[0] * a + off[0] * b + off[1] * c,
        off[0] * a + diag[1] * b + off[2] * c,
        off[1] * a + off[2] * b + diag[2] * c,
    )


def lift_kernel(probes_far, modulus_far, tangent_far, out, tangent, sems):
    count = probes_far.shape[0]
    core = lax.axis_index("core")
    copies = [
        pltpu.make_async_copy(probes_far.at[k, :, core], out.at[pl.ds(3 * k, 3)], sems.at[k]) for k in range(count)
    ]
    copies.append(pltpu.make_async_copy(modulus_far.at[pl.ds(core, 1)], out.at[pl.ds(3 * count, 1)], sems.at[count]))
    copies.append(pltpu.make_async_copy(tangent_far, tangent, sems.at[count + 1]))
    for copy in copies:
        copy.start()
    for copy in copies:
        copy.wait()


def partial_kernel(probes, modulus, tangent, far, near, prod):
    count = probes.shape[0]
    height = probes.shape[3]
    core = lax.axis_index("core")
    depth = (core, 1 - core)
    for z in range(2):
        for k in range(count):
            for i in range(3):
                prod[z * 3 * count + 3 * k + i] = probes[k, i, depth[z]] * modulus[depth[z]]
    for z, out in ((0, far), (1, near)):
        other = 1 - z
        for s in range(0, height, STRIP):
            here = pl.ds(s, STRIP)

            def mod(plane, shift):
                return rows_at(modulus, (depth[plane],), s, shift, height)

            m = mod(z, 0)
            side = mod(other, 0)
            neighbours = full_sum(m, mod(z, -1) + mod(z, 1), side, mod(other, -1) + mod(other, 1))
            common = (3.4 / 16.0) * m + PART * neighbours - 1.0
            diag = [common + 0.125 * tangent[i, depth[z], here, :] for i in range(3)]
            off = [0.125 * tangent[3 + i, depth[z], here, :] for i in range(3)]
            scaled = PART * m
            if z:
                out[6 * count, here, :] = m
            for k in range(count):
                values = [probes[k, i, depth[z], here, :] for i in range(3)]
                mixed = combine(diag, off, values)
                for i in range(3):
                    def val(plane, shift):
                        return rows_at(probes, (k, i, depth[plane]), s, shift, height)

                    def pro(plane, shift):
                        return rows_at(prod, (plane * 3 * count + 3 * k + i,), s, shift, height)

                    first = full_sum(values[i], val(z, -1) + val(z, 1), val(other, 0), val(other, -1) + val(other, 1))
                    second = full_sum(pro(z, 0), pro(z, -1) + pro(z, 1), pro(other, 0), pro(other, -1) + pro(other, 1))
                    if z:
                        out[3 * k + i, here, :] = values[i]
                    out[3 * count * z + 3 * k + i, here, :] = mixed[i] - scaled * first - PART * second


def filter_kernel(lo, lo_part, down, down_part, up, hi, tangent, out, once, prod, sums, products, prior):
    planes = (lo, down, up, hi)
    core = lax.axis_index("core")
    parts = (lo_part, down_part, up, hi)
    total = lo.shape[0] - 1
    count = total // 3
    height = lo.shape[1]
    blocks = height // STRIP
    last = (total, total, 2 * total, 2 * total)
    start = (0, 0, total, total)
    for z in range(4):
        for n in range(total):
            prior[z * total + n] = planes[z][n] * planes[z][last[z]]
    for source, target in ((0, 1), (1, 0), (2, 3), (3, 2)):
        src = planes[source]
        dst = planes[target]
        for s in range(0, height, STRIP):
            here = pl.ds(s, STRIP)

            def at(ref, n, shift):
                return rows_at(ref, (n,), s, shift, height)

            m = dst[last[target], here, :]
            weight = PART * outer_sum(*(at(src, last[source], d) for d in (0, -1, 1)))
            scaled = PART * m
            for n in range(total):
                first = outer_sum(at(src, n, 0), at(src, n, -1), at(src, n, 1))
                j = source * total + n
                second = outer_sum(at(prior, j, 0), at(prior, j, -1), at(prior, j, 1))
                value = parts[target][start[target] + n, here, :] + weight * dst[n, here, :] - scaled * first - PART * second
                if target in (0, 3):
                    value = jnp.where(m > 0.0, value, 0.0)
                once[target * total + n, here, :] = value
                prod[target * total + n, here, :] = value * m
    for z in (1, 2):
        for n in range(total):
            sums[(z - 1) * total + n] = once[(z - 1) * total + n] + once[(z + 1) * total + n]
            products[(z - 1) * total + n] = prod[(z - 1) * total + n] + prod[(z + 1) * total + n]
    for z, depth in ((1, core), (2, 1 - core)):
        plane = planes[z]
        for s in range(0, height, STRIP):
            here = pl.ds(s, STRIP)

            def at(ref, n, shift):
                return rows_at(ref, (n,), s, shift, height)

            def mod(p, shift):
                return rows_at(planes[p], (last[p],), s, shift, height)

            m = mod(z, 0)
            side = [mod(z - 1, d) + mod(z + 1, d) for d in (-1, 0, 1)]
            neighbours = full_sum(m, mod(z, -1) + mod(z, 1), side[1], side[0] + side[2])
            common = (6.8 / 16.0) * m + (2.0 * PART) * neighbours - 2.0
            diag = [common + 0.25 * tangent[i, depth, here, :] for i in range(3)]
            off = [0.25 * tangent[3 + i, depth, here, :] for i in range(3)]
            scaled = (2.0 * PART) * m
            turn = lax.rem(s // STRIP + blocks - lax.axis_index("probe"), blocks)
            for k in range(count):
                base = z * total + 3 * k
                mixed = combine(diag, off, [once[base + i, here, :] for i in range(3)])
                for i in range(3):
                    n = base + i
                    j = n - total
                    first = full_sum(at(once, n, 0), at(once, n, -1) + at(once, n, 1), at(sums, j, 0), at(sums, j, -1) + at(sums, j, 1))
                    second = full_sum(at(prod, n, 0), at(prod, n, -1) + at(prod, n, 1), at(products, j, 0), at(products, j, -1) + at(products, j, 1))
                    value = mixed[i] - scaled * first - (2.0 * PART) * second - plane[3 * k + i, here, :]
                    out[turn, k, i, depth] = value


def split(block):
    high = block.astype(jnp.bfloat16).astype(jnp.float32)
    rest = block - high
    middle = rest.astype(jnp.bfloat16).astype(jnp.float32)
    return high, middle, rest - middle


def piled(block):
    parts = list(split(block))
    if block.shape[0] % 16:
        parts.append(jnp.zeros_like(block))
    return jnp.concatenate(parts, axis=0).astype(jnp.bfloat16)


def folded(block, count, start, axis):
    pieces = [lax.slice_in_dim(block, start + n * count, start + (n + 1) * count, axis=axis) for n in range(3)]
    return (pieces[0] + pieces[1]) + pieces[2]


WIDE = 8


def gram_kernel(*refs, pieces, alone):
    stack, out, tall = refs[-3:]
    chunks = refs[: len(pieces)]
    earlier = refs[len(pieces) : -3]
    length = stack.shape[0]
    count = tall.shape[0] // length
    for chunk, (turn, first) in zip(chunks, pieces):
        each = chunk.shape[0]
        base = first
        if not alone:
            source = lax.axis_index("probe") - turn
            base = first + 2 * jnp.where(source < 0, source + count // 2, source)
        for j in range(each):
            tall[pl.ds(base + j, length, stride=count), :] = chunk[j]

    def step(r, gram):
        rows = []
        for h in range(WIDE):
            here = WIDE * r + h
            pile = piled(tall[pl.ds(here * count, count), :])
            stack[here] = pile
            rows.append(pile)
        own = jnp.concatenate(rows, axis=1)
        others = [jnp.concatenate([e[WIDE * r + h] for h in range(WIDE)], axis=1) for e in earlier]
        every = jnp.concatenate(others + [own], axis=0)
        return gram + lax.dot_general(own, every, (((1,), (1,)), ((), ())), preferred_element_type=jnp.float32)

    width = 3 * count * (1 + len(earlier))
    gram = lax.fori_loop(0, length // WIDE, step, jnp.zeros((3 * count, width), jnp.float32), unroll=2)
    gram = folded(gram, count, 0, 0)
    found = [folded(gram, count, 3 * count * n, 1) for n in range(1 + len(earlier))]
    if alone:
        found.append(jnp.zeros((count, count), jnp.float32))
    out[...] = jnp.concatenate(found, axis=1)


def pack_kernel(first, second, out):
    gram = jnp.concatenate([first[...], second[...]], axis=0)
    packed = jnp.concatenate([gram[8 * q : 8 * q + 8] for q in range(gram.shape[0] // 8)], axis=1)
    for n in range(out.shape[0]):
        out[n] = packed


def finish_kernel(copies, first, second, out, correlation, *, factor):
    length = first.shape[0]
    kept = first.shape[1] // 3
    made = second.shape[1] // 3
    total = kept + made
    summed = copies[0]
    for n in range(1, copies.shape[0]):
        summed = summed + copies[n]
    gram = jnp.concatenate([summed[:, total * q : total * q + total] for q in range(total // 8)], axis=0)
    row = lax.broadcasted_iota(jnp.int32, (total, total), 0)
    column = lax.broadcasted_iota(jnp.int32, (total, total), 1)
    unit = jnp.where(row == column, 1.0, 0.0)
    strict = jnp.where(row > column, gram, 0.0)
    mirrored = lax.dot_general(strict, unit, (((0,), (0,)), ((), ())), precision=lax.Precision.HIGHEST)
    gram = jnp.where(row >= column, gram, mirrored)
    work = jnp.concatenate([gram, unit, jnp.zeros((total, 128 - 2 * total), jnp.float32)], axis=1)
    slot = lax.broadcasted_iota(jnp.int32, (total, 1), 0)
    pivots = jnp.zeros((total, 1), jnp.float32)
    for k in range(total):
        if k == kept:
            correlation[...] = -factor * work[kept:, total : total + kept]
        pivot = work[k : k + 1, k : k + 1]
        ratio = jnp.where(slot > k, work[:, k : k + 1] / pivot, 0.0)
        pivots = jnp.where(slot == k, pivot, pivots)
        work = work - ratio * work[k : k + 1, :]
    weights = factor * work[kept:, total : 2 * total] * lax.rsqrt(pivots[kept:])
    there = lax.broadcasted_iota(jnp.int32, (made, made), 0)
    source = lax.broadcasted_iota(jnp.int32, (made, made), 1)
    moved = there + 2 * lax.axis_index("probe")
    turn = jnp.where(jnp.where(moved >= made, moved - made, moved) == source, 1.0, 0.0)
    weights = jnp.dot(turn, weights, precision=lax.Precision.HIGHEST)
    lines = []
    for part in split(weights):
        lines.append(jnp.concatenate([part[:, :kept]] * 3 + [part[:, kept:]] * 3, axis=1))
    left = jnp.concatenate(lines, axis=0).astype(jnp.bfloat16)
    for r in range(0, length, 2):
        sides = [jnp.concatenate([first[r + h], second[r + h]], axis=0) for h in range(2)]
        both = jnp.concatenate(sides, axis=1)
        wide_rows = lax.dot_general(left, both, (((1,), (0,)), ((), ())), preferred_element_type=jnp.float32)
        rows = (wide_rows[:made] + wide_rows[made : 2 * made]) + wide_rows[2 * made :]
        for h in range(2):
            out[pl.ds(r + h, made, stride=length), :] = rows[:, 128 * h : 128 * h + 128]


def out_turns(blocks):
    half = (len(blocks) - 1) // 2
    listed = []
    for n, block in enumerate(blocks):
        turn = n if n <= half else n - 1
        listed.append((block, turn, blocks[half].shape[0] if n == half + 1 else 0))
    return listed


def spread_kernel(*refs):
    blocks, out, sems = refs[:-2], refs[-2], refs[-1]
    turns = len(blocks) - 1
    copies = []
    for n, (block, k, first) in enumerate(out_turns(blocks)):
        source = lax.rem(lax.axis_index("probe") + turns - k, turns)
        target = out.at[pl.ds(first, block.shape[0]), :, :, pl.ds(source * STRIP, STRIP), :]
        copies.append(pltpu.make_async_copy(block, target, sems.at[n]))
    for copy in copies:
        copy.start()
    for copy in copies:
        copy.wait()


VM = pl.BlockSpec(memory_space=pltpu.VMEM)
FAR = pl.BlockSpec(memory_space=pltpu.HBM)


def near_chip(*arrays):
    return tuple(pltpu.with_memory_space_constraint(a, pltpu.VMEM) for a in arrays)


def in_far(*arrays):
    return tuple(pltpu.with_memory_space_constraint(a, pltpu.HBM) for a in arrays)


def lift_call(probes, modulus, tangent):
    count, _, _, height, breadth = probes.shape
    return pl.pallas_call(
        lift_kernel,
        out_shape=(
            pltpu.VMEM((3 * count + 1, height, breadth), jnp.float32),
            pltpu.VMEM(tangent.shape, jnp.float32),
        ),
        in_specs=[FAR] * 3,
        out_specs=(VM, VM),
        scratch_shapes=[pltpu.SemaphoreType.DMA((count + 2,))],
        compiler_params=pltpu.CompilerParams(vmem_limit_bytes=1 << 20),
        name="lift",
    )(*in_far(probes, modulus, tangent))


def partial_call(probes, modulus, tangent):
    count, _, _, height, breadth = probes.shape
    plane = lambda n: pltpu.VMEM((n, height, breadth), jnp.float32)
    return pl.pallas_call(
        partial_kernel,
        out_shape=(plane(3 * count), plane(6 * count + 1)),
        in_specs=[VM] * 3,
        out_specs=(VM, VM),
        scratch_shapes=[plane(6 * count)],
        compiler_params=pltpu.CompilerParams(vmem_limit_bytes=12 << 20),
        name="partial",
    )(*near_chip(probes, modulus, tangent))


def filter_call(packs, tangent):
    packed, height, breadth = packs[0].shape
    total = packed - 1
    plane = lambda n: pltpu.VMEM((n, height, breadth), jnp.float32)
    return pl.pallas_call(
        filter_kernel,
        out_shape=pltpu.VMEM((height // STRIP, total // 3, 3, 2, STRIP, breadth), jnp.float32),
        in_specs=[VM] * (len(packs) + 1),
        out_specs=VM,
        scratch_shapes=[plane(n * total) for n in (4, 4, 2, 2, 4)],
        compiler_params=pltpu.CompilerParams(vmem_limit_bytes=16 << 20),
        name="filter",
    )(*near_chip(*packs, tangent))


def gram_call(chunks, pieces, earlier=()):
    alone = not earlier
    length, breadth = chunks[0].shape[1:]
    count = sum(c.shape[0] for c in chunks)
    return pl.pallas_call(
        functools.partial(gram_kernel, pieces=pieces, alone=alone),
        out_shape=(
            pltpu.VMEM((length, 3 * count, breadth), jnp.bfloat16),
            pltpu.VMEM((count, 2 * count), jnp.float32),
        ),
        in_specs=[VM] * (len(chunks) + len(earlier)),
        out_specs=(VM, VM),
        scratch_shapes=[pltpu.VMEM((length * count, breadth), jnp.float32)],
        compiler_params=pltpu.CompilerParams(vmem_limit_bytes=8 << 20),
        name="gram",
    )(*near_chip(*chunks, *earlier))


def pack_call(grams, copies):
    total = grams[0].shape[1]
    return pl.pallas_call(
        pack_kernel,
        out_shape=pltpu.VMEM((copies, 8, total * total // 8), jnp.float32),
        in_specs=[VM] * 2,
        out_specs=VM,
        compiler_params=pltpu.CompilerParams(vmem_limit_bytes=4 << 20),
        name="pack",
    )(*near_chip(*grams))


def finish_call(copies, stacks, scale):
    length, _, breadth = stacks[0].shape
    return pl.pallas_call(
        functools.partial(finish_kernel, factor=scale),
        out_shape=(
            pltpu.VMEM((16 * length, breadth), jnp.float32),
            jax.ShapeDtypeStruct((16, 16), jnp.float32),
        ),
        in_specs=[VM] * 3,
        out_specs=(VM, VM),
        compiler_params=pltpu.CompilerParams(vmem_limit_bytes=8 << 20),
        name="finish",
    )(*near_chip(copies, *stacks))


def spread_call(blocks):
    count, parts, depth, strip, breadth = blocks[0].shape
    return pl.pallas_call(
        spread_kernel,
        out_shape=jax.ShapeDtypeStruct((count, parts, depth, strip * (len(blocks) - 1), breadth), jnp.float32),
        in_specs=[VM] * len(blocks),
        out_specs=FAR,
        scratch_shapes=[pltpu.SemaphoreType.DMA((len(blocks),))],
        compiler_params=pltpu.CompilerParams(vmem_limit_bytes=8 << 20),
        name="spread",
    )(*near_chip(*blocks))


def shift(block, by, columns):
    return lax.ppermute(block, "probe", [(j, (j + by) % columns) for j in range(columns)])


def exchange(parts, columns):
    half = columns // 2
    cut = parts[half].shape[0] // 2
    got = [parts[0]] + [None] * (columns - 1)
    ahead = shift(parts[half][:cut], half, columns)
    back = shift(parts[half][cut:], -(half // 2), columns)
    for k in range(1, columns):
        if k != half:
            got[k] = shift(parts[k], k, columns)
    back = shift(back, half // 2 - half, columns)
    return got[:half] + [ahead, back] + got[half + 1 :]


def body(probes, earlier, modulus, tangent, slabs, columns, scale):
    kept = earlier.shape[0]
    breadth = earlier.shape[-1]
    length = math.prod(earlier.shape[1:-1])
    places = ("x", "y", "core")
    outer = [(i, i + 1) for i in range(1, slabs - 1, 2)] + [(i, i - 1) for i in range(2, slabs, 2)]
    raw, tensor = lift_call(probes, modulus, tangent)
    got_raw = lax.ppermute(raw, places, outer)
    far, near = partial_call(probes, modulus, tensor)
    got_far = lax.ppermute(far, places, outer)
    got_near = lax.ppermute(near, "core", [(0, 1), (1, 0)])
    first, first_gram = gram_call([earlier.reshape(kept, length, breadth)], ((0, 0),))
    filtered = filter_call((got_raw, got_far, raw, far, near, got_near), tensor)
    got = exchange([filtered[k] for k in range(columns)], columns)
    half = columns // 2
    pieces = [(k, 0) for k in range(half + 1)] + [(half, 1)] + [(k, 0) for k in range(half + 1, columns)]
    flat = [g.reshape(g.shape[0], length, breadth) for g in got]
    second, second_gram = gram_call(flat, tuple(pieces), (first,))
    copies = pack_call((first_gram, second_gram), 2 * columns)
    copies = lax.all_to_all(copies, ("probe", "core"), 0, 0, tiled=True)
    copies = jnp.broadcast_to(jnp.sum(copies, axis=0, keepdims=True), (slabs // 2,) + copies.shape[1:])
    copies = lax.all_to_all(copies, ("x", "y"), 0, 0, tiled=True)
    rows, correlation = finish_call(copies, (first, second), scale)
    rows = rows.reshape((columns, 2) + earlier.shape[1:])
    got = exchange([rows[k] for k in range(columns)], columns)
    basis = spread_call(got)
    return (basis, correlation.T)


def solution(mesh):
    slabs = mesh.shape["slab"]
    columns = mesh.shape["probe"]
    side = math.isqrt(slabs // 2)
    wide = Mesh(mesh.devices.reshape(side, side, 2, columns), ("x", "y", "core", "probe"))
    slab = ("x", "y", "core")
    in_specs = (
        P("probe", None, slab, None, None),
        P(None, None, slab, "probe", None),
        P(slab, None, None),
        P(None, slab, None, None),
    )
    out_specs = (P("probe", None, slab, None, None), P())

    def step(probes, earlier, modulus, tangent):
        length = math.prod(probes.shape[1:])
        scale = math.sqrt(length)
        inner = lambda *parts: body(*parts, slabs, columns, scale)
        return jax.shard_map(inner, mesh=wide, in_specs=in_specs, out_specs=out_specs, check_vma=False)(
            probes, earlier, modulus, tangent
        )

    return step
```
